128 devices in a mesh: grp: 4 (over y), dev: 32 (over z, x, core).
Axes of the slice: x: 4, y: 4, z: 4, core: 2. Of those that a mesh axis runs over, the one named last changes fastest.
Arguments:
- ids: int32 [16384, 13, 2], P(('grp', 'dev')), may hold values from 0 to 262143, as said below
- location: int32 [262144], replicated, may hold values from 0 to 262143, as said below
- cold_table: bfloat16 [262144, 128], P(('grp', 'dev')), may hold values from -3 to 3
- hot_index: int32 [16384, 13], P(('grp', 'dev')), may hold values from 0 to 31
- hot_list: int32 [128, 32], P(('grp', 'dev')), may hold values from 0 to 4095, as said below
- hot_table: bfloat16 [4096, 128], replicated, may hold values from -3 to 3
- labels: int32 [16384], P(('grp', 'dev')), may hold values 0 or 1
- cross_u: bfloat16 [1664, 256], replicated, may hold values from -0.15625 to 0.15625
- cross_v: bfloat16 [256, 1664], replicated, may hold values from -0.375 to 0.375
- cross_bias: float32 [1664], replicated, may hold values from -3 to 3
- mlp_weight: bfloat16 [2048, 1664], replicated, may hold values from -0.15625 to 0.15625
- mlp_bias: float32 [2048], replicated, may hold values from -3 to 3
- out_weight: bfloat16 [2048], replicated, may hold values from -0.125 to 0.125
Outputs:
- cold_grad: float32 [262144, 128], P(('grp', 'dev'))
- hot_grad: float32 [4096, 128], replicated
- mlp_weight_grad: float32 [2048, 1664], P(('grp', 'dev'))
- cross_u_grad: float32 [1664, 256], replicated
- cross_v_grad: float32 [256, 1664], replicated
- cross_bias_grad: float32 [1664], replicated
- mlp_bias_grad: float32 [2048], replicated
- out_weight_grad: float32 [2048], replicated
The draws below stay inside these ranges and needn't reach their ends.
Inputs may be any that keep to these rules, and one draw needn't show every extreme that they name: The owner of an id is location[id] // 2048. Among the ids of one device's 128 samples (an aligned block of rows), at most 39 have any one owner; in every draw one owner has exactly 39 in every block. `location`: A permutation of 0 to 262143. `hot_list`: the 32 entries of each row are different.
All inputs are finite; a program needn't handle non-finite values. No bound on the sum of `labels` on one device may be relied on, other than what follows from the above.
Results may differ from the reference program's by a relative error of at most 0.0067.
Values may be sent and summed in bfloat16 or wider, within the bound.
No kernel may reach another device: no remote copies, remote signals or barrier semaphores. Data moves between devices by JAX's collectives and lax.ppermute only.
A program may use at most 128 MiB of HBM per device.

```python
import jax
import jax.numpy as jnp
from jax import lax

E = 128
F = 13
HOTS = 2
R = 256
H = 2048
HOT_ROWS = 4096
HOT_DEV = 32
SAMP_DEV = 128
SHARD_ROWS = 2048
DIN = 1664
SAMPLES = 16384
ROWS = 262144


def route_tables(key):
    devices = SAMPLES // SAMP_DEV
    per_device = SAMP_DEV * F * HOTS
    mean_load = per_device // devices
    spread = mean_load // 2
    place_key, owner_key, device_key = jax.random.split(jax.random.fold_in(key, 7), 3)
    location = jax.random.permutation(place_key, ROWS).astype(jnp.int32)
    inverse = jnp.zeros((ROWS,), jnp.int32).at[location].set(jnp.arange(ROWS, dtype=jnp.int32))
    full_owner = jax.random.randint(owner_key, (), 0, devices).astype(jnp.int32)

    def one_device(single_key):
        pair_key, diff_key, shuffle_key, slot_key = jax.random.split(single_key, 4)
        ranking = jax.random.permutation(pair_key, devices).astype(jnp.int32)
        leading = ranking[0]
        ranking = jnp.where(ranking == full_owner, leading, ranking).at[0].set(full_owner)
        offsets = jax.random.randint(diff_key, (devices // 2,), 0, spread + 1).astype(jnp.int32).at[0].set(spread)
        paired = jnp.stack([mean_load + offsets, mean_load - offsets], axis=1).reshape(devices)
        counts = jnp.zeros((devices,), jnp.int32).at[ranking].set(paired)
        owners = jnp.repeat(jnp.arange(devices, dtype=jnp.int32), counts, total_repeat_length=per_device)
        owners = jax.random.permutation(shuffle_key, owners)
        row_slot = jax.random.randint(slot_key, (per_device,), 0, SHARD_ROWS).astype(jnp.int32)
        return inverse[owners * SHARD_ROWS + row_slot]
    ids = jax.vmap(one_device)(jax.random.split(device_key, devices))
    return (location, ids.reshape(SAMPLES, F, HOTS).astype(jnp.int32))


def draw_ids(key, part):
    return route_tables(key)[1]


def draw_location(key, part):
    return route_tables(key)[0]


def draw_hot_list(key, part):
    devices = SAMPLES // SAMP_DEV
    row_keys = jax.random.split(jax.random.fold_in(key, 11), devices)

    def pick_rows(single_key):
        return jax.random.permutation(single_key, HOT_ROWS)[:HOT_DEV]
    return jax.vmap(pick_rows)(row_keys).astype(jnp.int32)


def touch_ends(drawn, stream_key, least, largest):
    shape = drawn.shape
    place = [jax.random.randint(jax.random.fold_in(stream_key, axis), (), 0, shape[axis]) for axis in range(len(shape))]
    drawn = drawn.at[tuple(place)].set(least)
    longest = shape.index(max(shape))
    place[longest] = (place[longest] + 1) % shape[longest]
    return drawn.at[tuple(place)].set(largest)


def block_levels(rng, extent, cuts, smallest, top_value):
    factor_of = 1.0
    for dim, shards_of in cuts:
        heights = jax.random.uniform(jax.random.fold_in(jax.random.fold_in(rng, 6), dim), (shards_of,), jnp.float32, smallest / len(cuts), top_value / len(cuts))
        factor_of = factor_of * jnp.repeat(jnp.exp(heights), extent[dim] // shards_of).reshape((-1,) + (1,) * (len(extent) - 1 - dim))
    return factor_of


def bell_draw(stream_key, dims, width, reach, shards=(), kind=jnp.bfloat16):
    drawn = width * jax.random.normal(stream_key, dims, jnp.float32)
    if shards:
        drawn = drawn * block_levels(stream_key, dims, shards, -0.22, 0.18)
    return jnp.clip(drawn, -reach, reach).astype(kind)


def setup_inputs(seed: int = 0) -> dict:
    streams_of = jax.random.split(jax.random.key(seed), 14)
    return {
        "ids": draw_ids(jax.random.fold_in(streams_of[13], 71), 0),
        "location": draw_location(jax.random.fold_in(streams_of[13], 71), 0),
        "cold_table": bell_draw(streams_of[2], (ROWS, E), 0.5, 3.0, ((0, 128),)),
        "hot_index": touch_ends(jax.random.randint(streams_of[3], (SAMPLES, F), 0, HOT_DEV), jax.random.fold_in(streams_of[3], 1), 0, HOT_DEV - 1).astype(jnp.int32),
        "hot_list": draw_hot_list(jax.random.fold_in(streams_of[13], 71), 0),
        "hot_table": bell_draw(streams_of[5], (HOT_ROWS, E), 0.5, 3.0),
        "labels": touch_ends((jax.random.randint(streams_of[6], (SAMPLES,), 0, 4) < 1).astype(jnp.int32), jax.random.fold_in(streams_of[6], 1), 0, 1),
        "cross_u": bell_draw(streams_of[7], (DIN, R), DIN ** -0.5, 0.15625),
        "cross_v": bell_draw(streams_of[8], (R, DIN), R ** -0.5, 0.375),
        "cross_bias": bell_draw(streams_of[9], (DIN,), 0.5, 3.0, (), jnp.float32),
        "mlp_weight": bell_draw(streams_of[10], (H, DIN), DIN ** -0.5, 0.15625),
        "mlp_bias": bell_draw(streams_of[11], (H,), 0.5, 3.0, (), jnp.float32),
        "out_weight": bell_draw(streams_of[12], (H,), H ** -0.5, 0.125),
    }


def silu_slope(values):
    squash = jax.nn.sigmoid(values)
    return squash * (1.0 + values * (1.0 - squash))


def contract_rows(former, latter):
    return lax.dot_general(former, latter, (((0,), (0,)), ((), ())), preferred_element_type=jnp.float32)


def contract_cols(former, latter):
    return lax.dot_general(former, latter, (((1,), (1,)), ((), ())), preferred_element_type=jnp.float32)


def reference(ids, location, cold_table, hot_index, hot_list, hot_table, labels, cross_u, cross_v, cross_bias, mlp_weight, mlp_bias, out_weight):
    blocks = SAMPLES // SAMP_DEV
    placed = location[ids].astype(jnp.int32)
    inputs = (placed.reshape(blocks, SAMP_DEV, F, HOTS), hot_index.reshape(blocks, SAMP_DEV, F), labels.reshape(blocks, SAMP_DEV), hot_list)

    def one_block(carried, pieces):
        block_place, block_index, block_label, block_list = pieces
        cold_rows = cold_table[block_place].astype(jnp.float32)
        pooled = jnp.sum(cold_rows, axis=2)
        hot_rows = block_list[block_index]
        pooled = pooled + hot_table[hot_rows].astype(jnp.float32)
        first_input = pooled.reshape(SAMP_DEV, F * E).astype(jnp.bfloat16)
        cross_low = jnp.dot(first_input, cross_u, preferred_element_type=jnp.float32).astype(jnp.bfloat16)
        cross_term = jnp.dot(cross_low, cross_v, preferred_element_type=jnp.float32) + cross_bias
        input_wide = first_input.astype(jnp.float32)
        cross_out = (input_wide * cross_term + input_wide).astype(jnp.bfloat16)
        hidden_in = contract_cols(cross_out, mlp_weight) + mlp_bias
        hidden = jax.nn.silu(hidden_in).astype(jnp.bfloat16)
        logits = jnp.dot(hidden, out_weight, preferred_element_type=jnp.float32)
        logit_grad = jax.nn.sigmoid(logits) - block_label.astype(jnp.float32)
        out_grad = jnp.dot(logit_grad, hidden.astype(jnp.float32), precision=lax.Precision.HIGHEST)
        hidden_grad = (logit_grad[:, None] * out_weight.astype(jnp.float32)[None, :] * silu_slope(hidden_in)).astype(jnp.bfloat16)
        bias_grad = jnp.sum(hidden_grad.astype(jnp.float32), axis=0)
        weight_grad = contract_rows(hidden_grad, cross_out)
        cross_out_grad = jnp.dot(hidden_grad, mlp_weight, preferred_element_type=jnp.float32)
        term_grad = (cross_out_grad * input_wide).astype(jnp.bfloat16)
        cross_bias_part = jnp.sum(term_grad.astype(jnp.float32), axis=0)
        cross_v_part = contract_rows(cross_low, term_grad)
        low_grad = contract_cols(term_grad, cross_v).astype(jnp.bfloat16)
        cross_u_part = contract_rows(first_input, low_grad)
        pooled_grad = (cross_out_grad * (cross_term + 1.0) + contract_cols(low_grad, cross_u)).astype(jnp.bfloat16)
        grad_wide = pooled_grad.astype(jnp.float32).reshape(SAMP_DEV, F, E)
        spread_rows = jnp.broadcast_to(grad_wide[:, :, None, :], (SAMP_DEV, F, HOTS, E)).reshape(SAMP_DEV * F * HOTS, E)
        cold_next = carried[6].at[block_place.reshape(SAMP_DEV * F * HOTS)].add(spread_rows)
        hot_next = carried[7].at[hot_rows.reshape(SAMP_DEV * F)].add(grad_wide.reshape(SAMP_DEV * F, E))
        updated = (carried[0] + cross_u_part, carried[1] + cross_v_part, carried[2] + cross_bias_part, carried[3] + bias_grad, carried[4] + out_grad, carried[5] + weight_grad, cold_next, hot_next)
        return updated, None

    initial = (jnp.zeros((F * E, R), jnp.float32), jnp.zeros((R, F * E), jnp.float32), jnp.zeros((F * E,), jnp.float32), jnp.zeros((H,), jnp.float32), jnp.zeros((H,), jnp.float32), jnp.zeros((H, F * E), jnp.float32), jnp.zeros((ROWS, E), jnp.float32), jnp.zeros((HOT_ROWS, E), jnp.float32))
    totals = lax.scan(one_block, initial, inputs)[0]
    return (totals[6], totals[7], totals[5], totals[0], totals[1], totals[2], totals[3], totals[4])
```

```python
import jax
import jax.numpy as jnp
from jax import lax
from jax.experimental import pallas as pl
from jax.experimental.pallas import tpu as pltpu
from jax.sharding import Mesh
from jax.sharding import PartitionSpec as P

GRP_DEV = ("grp", "dev_0", "dev_1", "dev_2")
CHIPS = ("grp", "dev_0", "dev_1")
CORE = "dev_2"
SWAP = [(0, 1), (1, 0)]
CAP = 40
HOT = 32
WAYS = 4
F32, BF16, I32 = jnp.float32, jnp.bfloat16, jnp.int32
VMEM = pl.BlockSpec(memory_space=pltpu.VMEM)
SMEM = pl.BlockSpec(memory_space=pltpu.SMEM)


def route_kernel(ids, hot_list, location, send, inverse, position, found):
    lane = lax.broadcasted_iota(I32, (1, 128), 1)
    rows = lax.broadcasted_iota(I32, (128, 128), 0)
    lanes = lax.broadcasted_iota(I32, (128, 128), 1)
    before = (lanes < rows).astype(BF16)
    diagonal = rows == lanes
    wide = lax.broadcasted_iota(I32, (128, 256), 1)
    wide_rank = wide & 63
    wide_part = wide >> 6
    wide_row = lax.broadcasted_iota(I32, (128, 256), 0)
    blocks = position.shape[0]
    features = blocks // 2

    def block(b, carried):
        seen, table = carried
        for j in range(128):
            number = ids[b, j]
            row = location[pl.ds(number >> 7, 1), :]
            found[pl.ds(j, 1), :] = jnp.where(lane == (number & 127), row, 0)
        placed = jnp.sum(found[...].astype(F32), axis=1, keepdims=True).astype(I32)
        owner = placed >> 11
        slot = (placed & 2047) + 1
        chosen = owner == lanes
        one_hot = chosen.astype(BF16)
        ahead = jnp.dot(before, one_hot, preferred_element_type=F32) + seen
        rank = jnp.sum(jnp.where(chosen, ahead, 0.0), axis=1, keepdims=True).astype(I32)
        seen = seen + jnp.sum(chosen.astype(F32), axis=0, keepdims=True)
        feature = jnp.where(b >= features, b - features, b)
        origin = feature * 128 + wide_row
        value = jnp.where(
            wide_part == 0,
            slot >> 4,
            jnp.where(
                wide_part == 1, slot & 15, jnp.where(wide_part == 2, origin >> 4, origin & 15)
            ),
        )
        value = jnp.where(wide_rank == rank, value, 0).astype(F32).astype(BF16)
        table = table + lax.dot_general(
            one_hot, value, (((0,), (0,)), ((), ())), preferred_element_type=F32
        )
        spot = jnp.where(diagonal, owner * CAP + rank, 0)
        position[pl.ds(b, 1), :] = jnp.sum(spot, axis=0, keepdims=True)
        return seen, table

    seen, table = lax.fori_loop(
        0, blocks, block, (jnp.zeros((1, 128), F32), jnp.zeros((128, 256), F32))
    )
    table = table.astype(I32)
    wanted = (table[:, :64] << 4) + table[:, 64:128] - 1
    wanted = jnp.where(wanted < 0, 2048, wanted)
    send[:, :CAP] = wanted[:, :CAP]
    send[:, CAP : CAP + 32] = jnp.broadcast_to(hot_list[...], (128, 32))
    send[:, CAP + 32 :] = jnp.zeros((128, 128 - CAP - 32), I32)
    inverse[...] = (table[:, 128:192] << 4) + table[:, 192:256]


def route(ids, hot_list, location):
    blocks = ids.shape[0]
    return pl.pallas_call(
        route_kernel,
        out_shape=(
            jax.ShapeDtypeStruct((128, 128), I32),
            jax.ShapeDtypeStruct((128, 64), I32),
            jax.ShapeDtypeStruct((blocks, 128), I32),
        ),
        in_specs=[SMEM, VMEM, VMEM],
        out_specs=(VMEM, VMEM, VMEM),
        scratch_shapes=[pltpu.VMEM((128, 128), I32)],
        name="route",
    )(ids, hot_list, location)


def fetch_kernel(wanted, table, out, wide, picked):
    shard = table.shape[0]
    wide[:shard, :] = table[...].astype(F32)
    wide[shard:, :] = jnp.zeros((8, 128), F32)

    def source(d, carried):
        for i in range(CAP):
            picked[pl.ds(d * CAP + i, 1), :] = wide[pl.ds(wanted[d, i], 1), :]
        return carried

    lax.fori_loop(0, out.shape[0] // CAP, source, 0)
    out[...] = picked[...].astype(BF16)


def fetch(wanted, table):
    count = wanted.shape[0] * CAP
    return pl.pallas_call(
        fetch_kernel,
        out_shape=jax.ShapeDtypeStruct((count, 128), BF16),
        in_specs=[SMEM, VMEM],
        out_specs=VMEM,
        scratch_shapes=[
            pltpu.VMEM((table.shape[0] + 8, 128), F32),
            pltpu.VMEM((count, 128), F32),
        ],
        name="fetch",
    )(wanted, table)


def cold_kernel(wanted, came, out, wide, *sums):
    for way in sums:
        way[...] = jnp.zeros(way.shape, F32)
    wide[...] = came[...].astype(F32)

    def source(d, carried):
        for i in range(CAP // WAYS):
            for k, way in enumerate(sums):
                at = k * (CAP // WAYS) + i
                here = pl.ds(wanted[d, at], 1)
                way[here, :] = way[here, :] + wide[d, at : at + 1, :]
        return carried

    lax.fori_loop(0, wide.shape[0], source, 0)
    shard = out.shape[0]
    total = sums[0][:shard, :]
    for way in sums[1:]:
        total = total + way[:shard, :]
    out[...] = total


def cold_sum(wanted, came, shard_rows):
    return pl.pallas_call(
        cold_kernel,
        out_shape=jax.ShapeDtypeStruct((shard_rows, 128), F32),
        in_specs=[SMEM, VMEM],
        out_specs=VMEM,
        scratch_shapes=[pltpu.VMEM(came.shape, F32)]
        + [pltpu.VMEM((shard_rows + 8, 128), F32)] * WAYS,
        name="cold_sum",
    )(wanted, came)


def hot_kernel(listed, came, out, wide):
    out[...] = jnp.zeros(out.shape, F32)
    wide[...] = came[...].astype(F32)

    def source(d, carried):
        places = [pl.ds(listed[d, CAP + i], 1) for i in range(HOT)]
        held = [out[here, :] + wide[d, i : i + 1, :] for i, here in enumerate(places)]
        for here, row in zip(places, held):
            out[here, :] = row
        return carried

    lax.fori_loop(0, came.shape[0], source, 0)


def hot_sum(listed, came, hot_rows):
    return pl.pallas_call(
        hot_kernel,
        out_shape=jax.ShapeDtypeStruct((hot_rows, 128), F32),
        in_specs=[SMEM, VMEM],
        out_specs=VMEM,
        scratch_shapes=[pltpu.VMEM(came.shape, F32)],
        name="hot_sum",
    )(listed, came)


def silu_slope(values):
    squash = jax.nn.sigmoid(values)
    return squash * (1.0 + values * (1.0 - squash))


def contract_rows(former, latter):
    return lax.dot_general(former, latter, (((0,), (0,)), ((), ())), preferred_element_type=F32)


def contract_cols(former, latter):
    return lax.dot_general(former, latter, (((1,), (1,)), ((), ())), preferred_element_type=F32)


def exchange(x, axes):
    return lax.all_to_all(x, axes, split_axis=0, concat_axis=0, tiled=True)


def by_core(x):
    return x.reshape(-1, 2, 16, *x.shape[1:]).swapaxes(0, 1).reshape(x.shape)


def from_core(x):
    return x.reshape(2, -1, 16).swapaxes(0, 1).reshape(-1)


def per_device(
    ids,
    location,
    cold_table,
    hot_index,
    hot_list,
    hot_table,
    labels,
    cross_u,
    cross_v,
    cross_bias,
    mlp_weight,
    mlp_bias,
    out_weight,
):
    devices = lax.axis_size(GRP_DEV)
    chips = lax.axis_size(CHIPS)
    samples, features, bag_size = ids.shape
    width = cold_table.shape[1]
    pairs = samples * features
    hidden_units, inputs = mlp_weight.shape
    rank = cross_u.shape[1]
    core = lax.axis_index(CORE)

    ids_rows = ids.transpose(2, 1, 0).reshape(bag_size * features, samples)
    send, inverse, position = route(ids_rows, hot_list, location.reshape(-1, 128))
    got = exchange(send.reshape(devices, 1, 128), GRP_DEV).reshape(devices, 128)
    rows = fetch(got, cold_table)
    arrived = exchange(rows.reshape(devices, CAP, width), GRP_DEV).reshape(devices * CAP, width)

    mlp_weight = by_core(mlp_weight)
    mlp_bias = by_core(mlp_bias)
    out_weight = by_core(out_weight)
    hot_pick = (
        hot_index.T.reshape(pairs)[:, None] == jnp.arange(HOT, dtype=I32)[None, :]
    ).astype(BF16)
    hot_part = jnp.dot(hot_pick, hot_table[hot_list[0]], preferred_element_type=F32)

    own = arrived[position.reshape(-1)].reshape(bag_size, pairs, width)
    pooled = own[0].astype(F32) + own[1].astype(F32) + hot_part
    first_input = (
        pooled.reshape(features, samples, width)
        .swapaxes(0, 1)
        .reshape(samples, inputs)
        .astype(BF16)
    )
    cross_low = jnp.dot(first_input, cross_u, preferred_element_type=F32).astype(BF16)
    cross_term = jnp.dot(cross_low, cross_v, preferred_element_type=F32) + cross_bias
    input_wide = first_input.astype(F32)
    cross_out = (input_wide * cross_term + input_wide).astype(BF16)
    hidden_in = contract_cols(cross_out, mlp_weight) + mlp_bias
    hidden = jax.nn.silu(hidden_in).astype(BF16)
    logits = jnp.dot(hidden, out_weight, preferred_element_type=F32)
    logit_grad = jax.nn.sigmoid(logits) - labels.astype(F32)
    out_grad = jnp.dot(logit_grad, hidden.astype(F32), precision=lax.Precision.HIGHEST)
    hidden_grad = (
        logit_grad[:, None] * out_weight.astype(F32)[None, :] * silu_slope(hidden_in)
    ).astype(BF16)
    bias_grad = jnp.sum(hidden_grad.astype(F32), axis=0)

    half = hidden_units // 2
    mine = lax.dynamic_slice(hidden_grad, (0, core * half), (samples, half))
    other = lax.dynamic_slice(hidden_grad, (0, (1 - core) * half), (samples, half))
    other = lax.ppermute(jnp.concatenate([other, cross_out], axis=1), CORE, SWAP)
    mlp_part = contract_rows(
        jnp.concatenate([mine, other[:, :half]], axis=0),
        jnp.concatenate([cross_out, other[:, half:]], axis=0),
    ).astype(BF16)
    mlp_parts = exchange(mlp_part.reshape(chips, half // chips, inputs), CHIPS)
    mlp_weight_grad = jnp.sum(mlp_parts.astype(F32), axis=0)

    cross_out_grad = jnp.dot(hidden_grad, mlp_weight, preferred_element_type=F32)
    term_grad = (cross_out_grad * input_wide).astype(BF16)
    cross_bias_part = jnp.sum(term_grad.astype(F32), axis=0)
    low_grad = contract_cols(term_grad, cross_v).astype(BF16)
    pooled_grad = (
        cross_out_grad * (cross_term + 1.0) + contract_cols(low_grad, cross_u)
    ).astype(BF16)

    grad_rows = pooled_grad.reshape(samples, features, width).swapaxes(0, 1).reshape(pairs, width)
    hot_block = contract_rows(hot_pick, grad_rows).astype(BF16)
    payload = jnp.concatenate(
        [
            grad_rows[inverse[:, :CAP].reshape(-1)].reshape(devices, CAP, width),
            jnp.broadcast_to(hot_block[None], (devices, HOT, width)),
        ],
        axis=1,
    )
    back = exchange(payload, GRP_DEV)
    cold_grad = cold_sum(got, back[:, :CAP], cold_table.shape[0])
    hot_grad = hot_sum(got, back[:, CAP:], hot_table.shape[0])

    first = core == 0
    pair_u = jnp.concatenate([low_grad, first_input], axis=1)
    pair_v = jnp.concatenate([cross_low, term_grad], axis=1)
    held = jnp.where(first, pair_u, pair_v)
    came = lax.ppermute(jnp.where(first, pair_v, pair_u), CORE, SWAP)
    both = jnp.concatenate([held, came], axis=0)
    cross_part = contract_rows(both[:, :rank], both[:, rank:])
    vectors = jnp.concatenate([cross_bias_part, bias_grad, out_grad])
    vector_rows = vectors.size // 128
    vectors = jnp.pad(vectors.reshape(vector_rows, 128), ((0, rank - vector_rows), (0, 0)))
    cross_part = jnp.concatenate([cross_part, vectors], axis=1).astype(BF16)
    cross_parts = exchange(cross_part.reshape(chips, rank // chips, inputs + 128), CHIPS)
    cross_sum = jnp.sum(cross_parts.astype(F32), axis=0).astype(BF16)
    cross_full = exchange(jnp.broadcast_to(cross_sum[None], cross_parts.shape), CHIPS)
    cross_full = cross_full.reshape(rank, inputs + 128)
    cross_other = lax.ppermute(cross_full, CORE, SWAP)
    cross_u_grad = jnp.where(first, cross_full, cross_other)[:, :inputs].astype(F32).T
    cross_v_grad = jnp.where(first, cross_other, cross_full)[:, :inputs].astype(F32)
    vectors = (
        cross_full[:vector_rows, inputs:].astype(F32)
        + cross_other[:vector_rows, inputs:].astype(F32)
    ).reshape(-1)
    return (
        cold_grad,
        hot_grad,
        mlp_weight_grad,
        cross_u_grad,
        cross_v_grad,
        vectors[:inputs],
        from_core(vectors[inputs : inputs + hidden_units]),
        from_core(vectors[inputs + hidden_units :]),
    )


def solution(mesh):
    torus = Mesh(
        mesh.devices.reshape(mesh.shape["grp"], 4, 4, 2), ("grp", "dev_0", "dev_1", "dev_2")
    )
    placed = (
        P(GRP_DEV, None, None),
        P(),
        P(GRP_DEV, None),
        P(GRP_DEV, None),
        P(GRP_DEV, None),
        P(),
        P(GRP_DEV),
        P(),
        P(),
        P(),
        P(),
        P(),
        P(),
    )
    return jax.shard_map(
        per_device,
        mesh=torus,
        in_specs=placed,
        out_specs=(P(GRP_DEV, None), P(), P(GRP_DEV, None), P(), P(), P(), P(), P()),
        check_vma=False,
    )
```

```python
import jax
import jax.numpy as jnp
from jax import lax
from jax.experimental import pallas as pl
from jax.experimental.pallas import tpu as pltpu
from jax.sharding import Mesh
from jax.sharding import PartitionSpec as P


GRP_DEV = ("grp", "dev_0", "dev_1", "dev_2")
CHIPS = ("grp", "dev_0", "dev_1")
CORE = "dev_2"
SWAP = [(0, 1), (1, 0)]
ORDER = ((2, 1, 0), (0, 2, 1))
CAP = 40
HOT = 32
WIDE = 512
WAYS = 8
F32, BF16, I32 = jnp.float32, jnp.bfloat16, jnp.int32
VMEM = pl.BlockSpec(memory_space=pltpu.VMEM)
SMEM = pl.BlockSpec(memory_space=pltpu.SMEM)


def spread(x, ones):
    return jnp.dot(x.astype(F32).astype(BF16), ones, preferred_element_type=F32).astype(I32)


def route_kernel(ids, hot_list, ids_lanes, location, send, inverse, position, found):
    blocks = position.shape[0]
    features = blocks // 2

    def pick(b, carried):
        for j in range(128):
            found[pl.ds(b * 128 + j, 1), :] = location[pl.ds(ids[b, j] >> 7, 1), :]
        return carried

    lax.fori_loop(0, blocks, pick, 0)
    rows = lax.broadcasted_iota(I32, (128, 128), 0)
    lanes = lax.broadcasted_iota(I32, (128, 128), 1)
    before = (lanes < rows).astype(BF16)
    diagonal = rows == lanes
    ones = jnp.ones((128, 128), BF16)
    low = [
        spread(jnp.where(diagonal, ids_lanes[b : b + 1, :] & 127, 0), ones) for b in range(blocks)
    ]
    value = [
        jnp.where(low[b] == lanes, found[b * 128 : (b + 1) * 128, :], 0) for b in range(blocks)
    ]
    owner = [spread(v >> 11, ones) for v in value]
    high = [spread((v & 2047) >> 4, ones) for v in value]
    deep = [spread(v & 15, ones) for v in value]
    chosen = [o == lanes for o in owner]
    one_hot = [c.astype(F32).astype(BF16) for c in chosen]
    ahead = [jnp.dot(before, o, preferred_element_type=F32) for o in one_hot]
    seen = jnp.zeros((1, 128), F32)
    table = jnp.zeros((128, 256), F32)
    lane_rank = lanes & 63
    left = lanes < 64
    for b in range(blocks):
        rank = spread(jnp.where(chosen[b], ahead[b] + seen, 0.0), ones)
        seen = seen + ahead[b][127:, :] + chosen[b][127:, :].astype(F32)
        hit = lane_rank == rank
        origin = (b % features) * 128 + rows
        slots = jnp.where(hit, jnp.where(left, high[b], deep[b]), 0)
        origins = jnp.where(hit, jnp.where(left, origin >> 4, origin & 15), 0)
        marks = jnp.concatenate(
            [slots.astype(F32).astype(BF16), origins.astype(F32).astype(BF16)], axis=1
        )
        table = table + contract_rows(one_hot[b], marks)
        spot = jnp.where(diagonal, owner[b] * CAP + rank, 0)
        position[b : b + 1, :] = jnp.sum(spot, axis=0, keepdims=True)
    table = table.astype(I32)
    held = spread(jnp.where(diagonal, jnp.broadcast_to(seen, (128, 128)), 0.0), ones)
    wanted = (table[:, :64] << 4) + table[:, 64:128]
    wanted = jnp.where(lanes[:, :64] < held[:, :64], wanted, 2048)
    send[:, :CAP] = wanted[:, :CAP]
    send[:, CAP : CAP + HOT] = jnp.broadcast_to(hot_list[...], (128, HOT))
    send[:, CAP + HOT :] = jnp.zeros((128, 128 - CAP - HOT), I32)
    inverse[...] = (table[:, 128:192] << 4) + table[:, 192:256]


def route(ids, hot_list, location):
    blocks = ids.shape[0]
    return pl.pallas_call(
        route_kernel,
        out_shape=(
            jax.ShapeDtypeStruct((128, 128), I32),
            jax.ShapeDtypeStruct((128, 64), I32),
            jax.ShapeDtypeStruct((blocks, 128), I32),
        ),
        in_specs=[SMEM, VMEM, VMEM, VMEM],
        out_specs=(VMEM, VMEM, VMEM),
        scratch_shapes=[pltpu.VMEM((blocks * 128, 128), I32)],
        name="route",
    )(ids, hot_list, ids, location)


def fetch_kernel(wanted, table, out, wide, picked):
    count, width = table.shape
    for f in range(width // 128):
        wide[f * count : (f + 1) * count, :] = table[:, f * 128 : (f + 1) * 128].astype(F32)
    wide[count * width // 128 :, :] = jnp.zeros((8, 128), F32)

    def source(d, carried):
        for i in range(CAP):
            picked[pl.ds(d * CAP + i, 1), :] = wide[pl.ds(wanted[d, i], 1), :]
        return carried

    lax.fori_loop(0, out.shape[0] // CAP, source, 0)
    out[...] = picked[...].astype(BF16)


def fetch(wanted, table):
    count = wanted.shape[0] * CAP
    return pl.pallas_call(
        fetch_kernel,
        out_shape=jax.ShapeDtypeStruct((count, 128), BF16),
        in_specs=[SMEM, VMEM],
        out_specs=VMEM,
        scratch_shapes=[
            pltpu.VMEM((table.size // 128 + 8, 128), F32),
            pltpu.VMEM((count, 128), F32),
        ],
        name="fetch",
    )(wanted, table)


def cold_kernel(wanted, came, out, wide, *sums):
    for way in sums:
        way[...] = jnp.zeros(way.shape, F32)
    wide[...] = came[...].astype(F32)

    def source(d, carried):
        for i in range(CAP // WAYS):
            for k, way in enumerate(sums):
                at = k * (CAP // WAYS) + i
                here = pl.ds(wanted[d, at], 1)
                way[here, :] = way[here, :] + wide[d, at : at + 1, :]
        return carried

    lax.fori_loop(0, wide.shape[0], source, 0)
    shard = out.shape[0]
    total = sums[0][:shard, :]
    for way in sums[1:]:
        total = total + way[:shard, :]
    out[...] = total


def cold_sum(wanted, came, shard_rows):
    return pl.pallas_call(
        cold_kernel,
        out_shape=jax.ShapeDtypeStruct((shard_rows, 128), F32),
        in_specs=[SMEM, VMEM],
        out_specs=VMEM,
        scratch_shapes=[pltpu.VMEM(came.shape, F32)]
        + [pltpu.VMEM((shard_rows + 8, 128), F32)] * WAYS,
        name="cold_sum",
    )(wanted, came)


def hot_kernel(listed, came, out, wide):
    out[...] = jnp.zeros(out.shape, F32)
    wide[...] = came[...].astype(F32)

    def source(d, carried):
        places = [pl.ds(listed[d, CAP + i], 1) for i in range(HOT)]
        held = [out[here, :] + wide[d, i : i + 1, :] for i, here in enumerate(places)]
        for here, row in zip(places, held):
            out[here, :] = row
        return carried

    lax.fori_loop(0, came.shape[0], source, 0)


def hot_sum(listed, came, hot_rows):
    return pl.pallas_call(
        hot_kernel,
        out_shape=jax.ShapeDtypeStruct((hot_rows, 128), F32),
        in_specs=[SMEM, VMEM],
        out_specs=VMEM,
        scratch_shapes=[pltpu.VMEM(came.shape, F32)],
        name="hot_sum",
    )(listed, came)


def unpack_kernel(core, held, came, u_out, v_out, bias_out, mlp_bias_out, out_weight_out, wide):
    first = core[0] == 0
    rank = v_out.shape[0]

    def block(c, chip, lanes):
        here = slice(chip * 16, (chip + 1) * 16)
        own, other = held[here, lanes].astype(F32), came[here, lanes].astype(F32)
        return jnp.where(first, own, other) if c == 0 else jnp.where(first, other, own)

    def chip_of(c, spot):
        place = [0, 0, 0]
        for axis, at in zip(ORDER[c], spot):
            place[axis] = at
        return (place[0] * 4 + place[1]) * 4 + place[2]

    blocks = rank // 16
    for q in range(4):
        count = WIDE if q < 3 else v_out.shape[1] - 3 * WIDE
        for r in range(blocks):
            spot = (q, r // 4, r % 4)
            rows = slice(r * 16, (r + 1) * 16)
            wide[rows, :count] = block(0, chip_of(0, spot), slice(0, count))
            v_out[rows, q * WIDE : q * WIDE + count] = block(1, chip_of(1, spot), slice(0, count))
        u_out[q * WIDE : q * WIDE + count, :] = wide[:, :count].T

    lanes = slice(128, 256)
    sums = jnp.concatenate(
        [
            block(0, chip_of(0, (3, r // 4, r % 4)), lanes)
            + block(1, chip_of(1, (3, r // 4, r % 4)), lanes)
            for r in range(3)
        ]
    )
    bias_out[...] = sums[: bias_out.shape[0]]
    start = bias_out.shape[0]
    for out in (mlp_bias_out, out_weight_out):
        tall = out.shape[0]
        part = sums[start : start + tall]
        start += tall
        for c in range(2):
            for at in range(64):
                spot = (at // 16, at // 4 % 4, at % 4)
                chip = chip_of(c, spot)
                come, go = c * 64 + at, chip * 2 + c
                out[go // 8 : go // 8 + 1, go % 8 * 16 : go % 8 * 16 + 16] = part[
                    come // 8 : come // 8 + 1, come % 8 * 16 : come % 8 * 16 + 16
                ]


def unpack(core, held, came, inputs, rank, hidden_units):
    return pl.pallas_call(
        unpack_kernel,
        out_shape=(
            jax.ShapeDtypeStruct((inputs, rank), F32),
            jax.ShapeDtypeStruct((rank, inputs), F32),
            jax.ShapeDtypeStruct((inputs // 128, 128), F32),
            jax.ShapeDtypeStruct((hidden_units // 128, 128), F32),
            jax.ShapeDtypeStruct((hidden_units // 128, 128), F32),
        ),
        in_specs=[SMEM, VMEM, VMEM],
        out_specs=(VMEM,) * 5,
        scratch_shapes=[pltpu.VMEM((rank, WIDE), F32)],
        name="unpack",
    )(core.reshape(1), held, came)


def silu_slope(values):
    squash = jax.nn.sigmoid(values)
    return squash * (1.0 + values * (1.0 - squash))


def contract_rows(former, latter):
    return lax.dot_general(former, latter, (((0,), (0,)), ((), ())), preferred_element_type=F32)


def contract_cols(former, latter):
    return lax.dot_general(former, latter, (((1,), (1,)), ((), ())), preferred_element_type=F32)


def exchange(x, axes):
    return lax.all_to_all(x, axes, split_axis=0, concat_axis=0, tiled=True)


def route_pairs(phase, shift):
    pairs = []
    for d in range(128):
        spot = [d // 32, d // 8 % 4, d // 2 % 4]
        axis = ORDER[d % 2][phase]
        spot[axis] = (spot[axis] + shift) % 4
        pairs.append((d, ((spot[0] * 4 + spot[1]) * 4 + spot[2]) * 2 + d % 2))
    return pairs


def scatter_phase(x, phase, core):
    here = jnp.where(
        core == 0, lax.axis_index(CHIPS[ORDER[0][phase]]), lax.axis_index(CHIPS[ORDER[1][phase]])
    )
    tiles = x.reshape(4, -1, x.shape[-1])
    came = [
        lax.ppermute(
            lax.dynamic_index_in_dim(tiles, (here + s) % 4, 0, False),
            GRP_DEV,
            route_pairs(phase, s),
        )
        for s in (1, 3, 2)
    ]
    total = lax.dynamic_index_in_dim(tiles, here, 0, False).astype(F32)
    for tile in came:
        total = total + tile.astype(F32)
    return total


def by_core(x):
    parts = x.reshape(4, 4, 4, 2, 16, *x.shape[1:])
    halves = []
    for c in range(2):
        rest = tuple(range(3, 3 + x.ndim))
        half = parts[:, :, :, c].transpose(*ORDER[c], *rest)
        halves.append(half.reshape(-1, *x.shape[1:]))
    return jnp.concatenate(halves)


def per_device(
    ids,
    location,
    cold_table,
    hot_index,
    hot_list,
    hot_table,
    labels,
    cross_u,
    cross_v,
    cross_bias,
    mlp_weight,
    mlp_bias,
    out_weight,
):
    devices = lax.axis_size(GRP_DEV)
    chips = lax.axis_size(CHIPS)
    samples, features, bag_size = ids.shape
    width = cold_table.shape[1]
    pairs = samples * features
    hidden_units, inputs = mlp_weight.shape
    rank = cross_u.shape[1]
    core = lax.axis_index(CORE)

    ids_rows = ids.transpose(2, 1, 0).reshape(bag_size * features, samples)
    send, inverse, position = route(ids_rows, hot_list, location.reshape(-1, 128))
    got = exchange(send.reshape(devices, 1, 128), GRP_DEV).reshape(devices, 128)
    rows = fetch(got, cold_table)
    arrived = exchange(rows.reshape(devices, CAP, width), GRP_DEV).reshape(devices * CAP, width)

    mlp_weight = by_core(mlp_weight)
    mlp_bias = by_core(mlp_bias)
    out_weight = by_core(out_weight)
    hot_pick = (
        hot_index.T.reshape(pairs)[:, None] == jnp.arange(HOT, dtype=I32)[None, :]
    ).astype(BF16)
    hot_part = jnp.dot(hot_pick, hot_table[hot_list[0]], preferred_element_type=F32)

    own = arrived[position.reshape(-1)].reshape(bag_size, pairs, width)
    pooled = own[0].astype(F32) + own[1].astype(F32) + hot_part
    first_input = (
        pooled.reshape(features, samples, width)
        .swapaxes(0, 1)
        .reshape(samples, inputs)
        .astype(BF16)
    )
    cross_low = jnp.dot(first_input, cross_u, preferred_element_type=F32).astype(BF16)
    cross_term = jnp.dot(cross_low, cross_v, preferred_element_type=F32) + cross_bias
    input_wide = first_input.astype(F32)
    cross_out = (input_wide * cross_term + input_wide).astype(BF16)
    hidden_in = contract_cols(cross_out, mlp_weight) + mlp_bias
    hidden = jax.nn.silu(hidden_in).astype(BF16)
    logits = jnp.dot(hidden, out_weight, preferred_element_type=F32)
    logit_grad = jax.nn.sigmoid(logits) - labels.astype(F32)
    out_grad = jnp.dot(logit_grad, hidden.astype(F32), precision=lax.Precision.HIGHEST)
    hidden_grad = (
        logit_grad[:, None] * out_weight.astype(F32)[None, :] * silu_slope(hidden_in)
    ).astype(BF16)
    bias_grad = jnp.sum(hidden_grad.astype(F32), axis=0)

    half = hidden_units // 2
    mine = lax.dynamic_slice(hidden_grad, (0, core * half), (samples, half))
    other = lax.dynamic_slice(hidden_grad, (0, (1 - core) * half), (samples, half))
    other = lax.ppermute(jnp.concatenate([other, cross_out], axis=1), CORE, SWAP)
    mlp_part = contract_rows(
        jnp.concatenate([mine, other[:, :half]], axis=0),
        jnp.concatenate([cross_out, other[:, half:]], axis=0),
    ).astype(BF16)

    cross_out_grad = jnp.dot(hidden_grad, mlp_weight, preferred_element_type=F32)
    term_grad = (cross_out_grad * input_wide).astype(BF16)
    cross_bias_part = jnp.sum(term_grad.astype(F32), axis=0)
    low_grad = contract_cols(term_grad, cross_v).astype(BF16)
    pooled_grad = (
        cross_out_grad * (cross_term + 1.0) + contract_cols(low_grad, cross_u)
    ).astype(BF16)

    mlp_sum = scatter_phase(mlp_part, 0, core).astype(BF16)

    first = core == 0
    pair_u = jnp.concatenate([low_grad, first_input], axis=1)
    pair_v = jnp.concatenate([cross_low, term_grad], axis=1)
    held = jnp.where(first, pair_u, pair_v)
    came = lax.ppermute(jnp.where(first, pair_v, pair_u), CORE, SWAP)
    both = jnp.concatenate([held, came], axis=0)
    cross_part = contract_rows(both[:, :rank], both[:, rank:])
    vectors = jnp.concatenate([cross_bias_part, bias_grad, out_grad])
    vector_rows = vectors.size // 128
    vectors = jnp.pad(
        vectors.reshape(vector_rows, 128), ((0, rank - vector_rows), (0, 4 * WIDE - inputs - 128))
    )
    cross_part = jnp.concatenate(
        [cross_part[:, q * WIDE : (q + 1) * WIDE] for q in range(3)]
        + [jnp.concatenate([cross_part[:, 3 * WIDE :], vectors], axis=1)],
        axis=0,
    ).astype(BF16)
    cross_sum = scatter_phase(cross_part, 0, core).astype(BF16)

    grad_rows = pooled_grad.reshape(samples, features, width).swapaxes(0, 1).reshape(pairs, width)
    hot_block = contract_rows(hot_pick, grad_rows).astype(BF16)
    payload = jnp.concatenate(
        [
            fetch(inverse, pooled_grad).reshape(devices, CAP, width),
            jnp.broadcast_to(hot_block[None], (devices, HOT, width)),
        ],
        axis=1,
    )
    back = exchange(payload, GRP_DEV)

    sums = scatter_phase(jnp.concatenate([mlp_sum, cross_sum], axis=1), 1, core)
    sums = scatter_phase(sums, 2, core)
    mlp_weight_grad = sums[:, :inputs]
    shared = jnp.broadcast_to(sums[None, :, inputs:].astype(BF16), (chips, 16, WIDE))
    shared, back = lax.optimization_barrier((shared, back))
    shared = exchange(shared, CHIPS).reshape(-1, WIDE)
    cold_grad = cold_sum(got, back[:, :CAP], cold_table.shape[0])
    hot_grad = hot_sum(got, back[:, CAP:], hot_table.shape[0])
    other_shared = lax.ppermute(shared, CORE, SWAP)
    cross_u_grad, cross_v_grad, cross_bias_grad, mlp_bias_grad, out_weight_grad = unpack(
        core, shared, other_shared, inputs, rank, hidden_units
    )
    return (
        cold_grad,
        hot_grad,
        mlp_weight_grad,
        cross_u_grad,
        cross_v_grad,
        cross_bias_grad.reshape(-1),
        mlp_bias_grad.reshape(-1),
        out_weight_grad.reshape(-1),
    )


def solution(mesh):
    torus = Mesh(
        mesh.devices.reshape(mesh.shape["grp"], 4, 4, 2), ("grp", "dev_0", "dev_1", "dev_2")
    )
    placed = (
        P(GRP_DEV, None, None),
        P(),
        P(GRP_DEV, None),
        P(GRP_DEV, None),
        P(GRP_DEV, None),
        P(),
        P(GRP_DEV),
        P(),
        P(),
        P(),
        P(),
        P(),
        P(),
    )
    return jax.shard_map(
        per_device,
        mesh=torus,
        in_specs=placed,
        out_specs=(P(GRP_DEV, None), P(), P(GRP_DEV, None), P(), P(), P(), P(), P()),
        check_vma=False,
    )
```

```python
import jax
import jax.numpy as jnp
from jax import lax
from jax.experimental import pallas as pl
from jax.experimental.pallas import tpu as pltpu
from jax.sharding import Mesh
from jax.sharding import PartitionSpec as P


GRP_DEV = ("grp", "dev_0", "dev_1", "dev_2")
CHIPS = ("grp", "dev_0", "dev_1")
CORE = "dev_2"
SWAP = [(0, 1), (1, 0)]
ORDER = ((2, 1, 0), (0, 2, 1))
CAP = 40
HOT = 32
WIDE = 512
WAYS = 8
F32, BF16, I32 = jnp.float32, jnp.bfloat16, jnp.int32
VMEM = pl.BlockSpec(memory_space=pltpu.VMEM)
SMEM = pl.BlockSpec(memory_space=pltpu.SMEM)


def spread(x, ones):
    return jnp.dot(x.astype(F32).astype(BF16), ones, preferred_element_type=F32).astype(I32)


def route_kernel(ids, hot_list, ids_lanes, location, send, inverse, position, found):
    blocks = position.shape[0]
    features = blocks // 2

    def pick(b, carried):
        for j in range(128):
            found[pl.ds(b * 128 + j, 1), :] = location[pl.ds(ids[b, j] >> 7, 1), :]
        return carried

    lax.fori_loop(0, blocks, pick, 0)
    rows = lax.broadcasted_iota(I32, (128, 128), 0)
    lanes = lax.broadcasted_iota(I32, (128, 128), 1)
    before = (lanes < rows).astype(BF16)
    diagonal = rows == lanes
    ones = jnp.ones((128, 128), BF16)
    low = [
        spread(jnp.where(diagonal, ids_lanes[b : b + 1, :] & 127, 0), ones) for b in range(blocks)
    ]
    value = [
        jnp.where(low[b] == lanes, found[b * 128 : (b + 1) * 128, :], 0) for b in range(blocks)
    ]
    owner = [spread(v >> 11, ones) for v in value]
    high = [spread((v & 2047) >> 4, ones) for v in value]
    deep = [spread(v & 15, ones) for v in value]
    chosen = [o == lanes for o in owner]
    one_hot = [c.astype(F32).astype(BF16) for c in chosen]
    ahead = [jnp.dot(before, o, preferred_element_type=F32) for o in one_hot]
    seen = jnp.zeros((1, 128), F32)
    table = jnp.zeros((128, 256), F32)
    lane_rank = lanes & 63
    left = lanes < 64
    for b in range(blocks):
        rank = spread(jnp.where(chosen[b], ahead[b] + seen, 0.0), ones)
        seen = seen + ahead[b][127:, :] + chosen[b][127:, :].astype(F32)
        hit = lane_rank == rank
        origin = (b % features) * 128 + rows
        slots = jnp.where(hit, jnp.where(left, high[b], deep[b]), 0)
        origins = jnp.where(hit, jnp.where(left, origin >> 4, origin & 15), 0)
        marks = jnp.concatenate(
            [slots.astype(F32).astype(BF16), origins.astype(F32).astype(BF16)], axis=1
        )
        table = table + contract_rows(one_hot[b], marks)
        spot = jnp.where(diagonal, owner[b] * CAP + rank, 0)
        position[b : b + 1, :] = jnp.sum(spot, axis=0, keepdims=True)
    table = table.astype(I32)
    held = spread(jnp.where(diagonal, jnp.broadcast_to(seen, (128, 128)), 0.0), ones)
    wanted = (table[:, :64] << 4) + table[:, 64:128]
    wanted = jnp.where(lanes[:, :64] < held[:, :64], wanted, 2048)
    send[:, :CAP] = wanted[:, :CAP]
    send[:, CAP : CAP + HOT] = jnp.broadcast_to(hot_list[...], (128, HOT))
    send[:, CAP + HOT :] = jnp.zeros((128, 128 - CAP - HOT), I32)
    inverse[...] = (table[:, 128:192] << 4) + table[:, 192:256]


def route(ids, hot_list, location):
    blocks = ids.shape[0]
    return pl.pallas_call(
        route_kernel,
        out_shape=(
            jax.ShapeDtypeStruct((128, 128), I32),
            jax.ShapeDtypeStruct((128, 64), I32),
            jax.ShapeDtypeStruct((blocks, 128), I32),
        ),
        in_specs=[SMEM, VMEM, VMEM, VMEM],
        out_specs=(VMEM, VMEM, VMEM),
        scratch_shapes=[pltpu.VMEM((blocks * 128, 128), I32)],
        name="route",
    )(ids, hot_list, ids, location)


def fetch_kernel(wanted, table, out, wide, picked):
    shard = table.shape[0]
    wide[:shard, :] = table[...].astype(F32)
    wide[shard:, :] = jnp.zeros((8, 128), F32)

    def source(d, carried):
        for i in range(CAP):
            picked[pl.ds(d * CAP + i, 1), :] = wide[pl.ds(wanted[d, i], 1), :]
        return carried

    lax.fori_loop(0, out.shape[0] // CAP, source, 0)
    out[...] = picked[...].astype(BF16)


def fetch(wanted, table):
    count = wanted.shape[0] * CAP
    return pl.pallas_call(
        fetch_kernel,
        out_shape=jax.ShapeDtypeStruct((count, 128), BF16),
        in_specs=[SMEM, VMEM],
        out_specs=VMEM,
        scratch_shapes=[
            pltpu.VMEM((table.shape[0] + 8, 128), F32),
            pltpu.VMEM((count, 128), F32),
        ],
        name="fetch",
    )(wanted, table)


def pool_kernel(position, hot_index, hot_rows, arrived, out, wide, total):
    features, samples = hot_index.shape
    wide[...] = arrived[...].astype(F32)
    slots = lax.broadcasted_iota(I32, (HOT, samples), 0)

    def feature(f, carried):
        for s in range(samples):
            total[s : s + 1, :] = (
                wide[pl.ds(position[f, s], 1), :] + wide[pl.ds(position[features + f, s], 1), :]
            )
        picked = (slots == hot_index[pl.ds(f, 1), :]).astype(F32).astype(BF16)
        both = total[...] + contract_rows(picked, hot_rows[...])
        out[:, pl.ds(pl.multiple_of(f * 128, 128), 128)] = both.astype(BF16)
        return carried

    lax.fori_loop(0, features, feature, 0)


def pool(position, hot_index, hot_rows, arrived):
    features, samples = hot_index.shape
    return pl.pallas_call(
        pool_kernel,
        out_shape=jax.ShapeDtypeStruct((samples, features * 128), BF16),
        in_specs=[SMEM, VMEM, VMEM, VMEM],
        out_specs=VMEM,
        scratch_shapes=[pltpu.VMEM(arrived.shape, F32), pltpu.VMEM((samples, 128), F32)],
        name="pool",
    )(position, hot_index, hot_rows, arrived)


def pack_kernel(inverse, hot_index, grad, out, wide, picked):
    samples, inputs = grad.shape
    devices = out.shape[0]
    slots = lax.broadcasted_iota(I32, (HOT, samples), 0)
    hot_block = jnp.zeros((HOT, 128), F32)
    for f in range(inputs // 128):
        part = grad[:, f * 128 : (f + 1) * 128]
        wide[f * samples : (f + 1) * samples, :] = part.astype(F32)
        one_hot = (slots == hot_index[f : f + 1, :]).astype(F32).astype(BF16)
        hot_block = hot_block + jnp.dot(one_hot, part, preferred_element_type=F32)

    def source(d, carried):
        for i in range(CAP):
            picked[pl.ds(d * CAP + i, 1), :] = wide[pl.ds(inverse[d, i], 1), :]
        return carried

    lax.fori_loop(0, devices, source, 0)
    out[:, :CAP, :] = picked[...].reshape(devices, CAP, 128).astype(BF16)
    out[:, CAP:, :] = jnp.broadcast_to(hot_block.astype(BF16)[None], (devices, HOT, 128))


def pack(inverse, hot_index, grad):
    devices = inverse.shape[0]
    return pl.pallas_call(
        pack_kernel,
        out_shape=jax.ShapeDtypeStruct((devices, CAP + HOT, 128), BF16),
        in_specs=[SMEM, VMEM, VMEM],
        out_specs=VMEM,
        scratch_shapes=[
            pltpu.VMEM((grad.size // 128, 128), F32),
            pltpu.VMEM((devices * CAP, 128), F32),
        ],
        name="pack",
    )(inverse, hot_index, grad)


def cold_kernel(wanted, came, out, wide, *sums):
    for way in sums:
        way[...] = jnp.zeros(way.shape, F32)
    wide[...] = came[:, :CAP, :].astype(F32)

    def source(d, carried):
        for i in range(CAP // WAYS):
            for k, way in enumerate(sums):
                at = k * (CAP // WAYS) + i
                here = pl.ds(wanted[d, at], 1)
                way[here, :] = way[here, :] + wide[d, at : at + 1, :]
        return carried

    lax.fori_loop(0, wide.shape[0], source, 0)
    shard = out.shape[0]
    total = sums[0][:shard, :]
    for way in sums[1:]:
        total = total + way[:shard, :]
    out[...] = total


def cold_sum(wanted, came, shard_rows):
    return pl.pallas_call(
        cold_kernel,
        out_shape=jax.ShapeDtypeStruct((shard_rows, 128), F32),
        in_specs=[SMEM, VMEM],
        out_specs=VMEM,
        scratch_shapes=[pltpu.VMEM((came.shape[0], CAP, 128), F32)]
        + [pltpu.VMEM((shard_rows + 8, 128), F32)] * WAYS,
        name="cold_sum",
    )(wanted, came)


def hot_kernel(listed, came, out, wide):
    out[...] = jnp.zeros(out.shape, F32)
    wide[...] = came[:, CAP:, :].astype(F32)

    def source(d, carried):
        places = [pl.ds(listed[d, CAP + i], 1) for i in range(HOT)]
        held = [out[here, :] + wide[d, i : i + 1, :] for i, here in enumerate(places)]
        for here, row in zip(places, held):
            out[here, :] = row
        return carried

    lax.fori_loop(0, came.shape[0], source, 0)


def hot_sum(listed, came, hot_rows):
    return pl.pallas_call(
        hot_kernel,
        out_shape=jax.ShapeDtypeStruct((hot_rows, 128), F32),
        in_specs=[SMEM, VMEM],
        out_specs=VMEM,
        scratch_shapes=[pltpu.VMEM((came.shape[0], HOT, 128), F32)],
        name="hot_sum",
    )(listed, came)


def unpack_kernel(core, held, came, u_out, v_out, bias_out, mlp_bias_out, out_weight_out, wide):
    first = core[0] == 0
    rank = v_out.shape[0]

    def block(c, chip, lanes):
        here = slice(chip * 16, (chip + 1) * 16)
        own, other = held[here, lanes].astype(F32), came[here, lanes].astype(F32)
        return jnp.where(first, own, other) if c == 0 else jnp.where(first, other, own)

    def chip_of(c, spot):
        place = [0, 0, 0]
        for axis, at in zip(ORDER[c], spot):
            place[axis] = at
        return (place[0] * 4 + place[1]) * 4 + place[2]

    blocks = rank // 16
    for q in range(4):
        count = WIDE if q < 3 else v_out.shape[1] - 3 * WIDE
        for r in range(blocks):
            spot = (q, r // 4, r % 4)
            rows = slice(r * 16, (r + 1) * 16)
            wide[rows, :count] = block(0, chip_of(0, spot), slice(0, count))
            v_out[rows, q * WIDE : q * WIDE + count] = block(1, chip_of(1, spot), slice(0, count))
        u_out[q * WIDE : q * WIDE + count, :] = wide[:, :count].T

    lanes = slice(128, 256)
    sums = jnp.concatenate(
        [
            block(0, chip_of(0, (3, r // 4, r % 4)), lanes)
            + block(1, chip_of(1, (3, r // 4, r % 4)), lanes)
            for r in range(3)
        ]
    )
    bias_out[...] = sums[: bias_out.shape[0]]
    start = bias_out.shape[0]
    for out in (mlp_bias_out, out_weight_out):
        tall = out.shape[0]
        part = sums[start : start + tall]
        start += tall
        for c in range(2):
            for at in range(64):
                spot = (at // 16, at // 4 % 4, at % 4)
                chip = chip_of(c, spot)
                come, go = c * 64 + at, chip * 2 + c
                out[go // 8 : go // 8 + 1, go % 8 * 16 : go % 8 * 16 + 16] = part[
                    come // 8 : come // 8 + 1, come % 8 * 16 : come % 8 * 16 + 16
                ]


def unpack(core, held, came, inputs, rank, hidden_units):
    return pl.pallas_call(
        unpack_kernel,
        out_shape=(
            jax.ShapeDtypeStruct((inputs, rank), F32),
            jax.ShapeDtypeStruct((rank, inputs), F32),
            jax.ShapeDtypeStruct((inputs // 128, 128), F32),
            jax.ShapeDtypeStruct((hidden_units // 128, 128), F32),
            jax.ShapeDtypeStruct((hidden_units // 128, 128), F32),
        ),
        in_specs=[SMEM, VMEM, VMEM],
        out_specs=(VMEM,) * 5,
        scratch_shapes=[pltpu.VMEM((rank, WIDE), F32)],
        name="unpack",
    )(core.reshape(1), held, came)


def silu_slope(values):
    squash = jax.nn.sigmoid(values)
    return squash * (1.0 + values * (1.0 - squash))


def contract_rows(former, latter):
    return lax.dot_general(former, latter, (((0,), (0,)), ((), ())), preferred_element_type=F32)


def contract_cols(former, latter):
    return lax.dot_general(former, latter, (((1,), (1,)), ((), ())), preferred_element_type=F32)


def exchange(x, axes):
    return lax.all_to_all(x, axes, split_axis=0, concat_axis=0, tiled=True)


def route_pairs(phase, shift):
    pairs = []
    for d in range(128):
        spot = [d // 32, d // 8 % 4, d // 2 % 4]
        axis = ORDER[d % 2][phase]
        spot[axis] = (spot[axis] + shift) % 4
        pairs.append((d, ((spot[0] * 4 + spot[1]) * 4 + spot[2]) * 2 + d % 2))
    return pairs


def scatter_phase(x, phase, core):
    here = jnp.where(
        core == 0, lax.axis_index(CHIPS[ORDER[0][phase]]), lax.axis_index(CHIPS[ORDER[1][phase]])
    )
    tiles = x.reshape(4, -1, x.shape[-1])
    came = [
        lax.ppermute(
            lax.dynamic_index_in_dim(tiles, (here + s) % 4, 0, False),
            GRP_DEV,
            route_pairs(phase, s),
        )
        for s in (1, 3, 2)
    ]
    total = lax.dynamic_index_in_dim(tiles, here, 0, False).astype(F32)
    for tile in came:
        total = total + tile.astype(F32)
    return total


def by_core(x):
    parts = x.reshape(4, 4, 4, 2, 16, *x.shape[1:])
    halves = []
    for c in range(2):
        rest = tuple(range(3, 3 + x.ndim))
        half = parts[:, :, :, c].transpose(*ORDER[c], *rest)
        halves.append(half.reshape(-1, *x.shape[1:]))
    return jnp.concatenate(halves)


def per_device(
    ids,
    location,
    cold_table,
    hot_index,
    hot_list,
    hot_table,
    labels,
    cross_u,
    cross_v,
    cross_bias,
    mlp_weight,
    mlp_bias,
    out_weight,
):
    devices = lax.axis_size(GRP_DEV)
    chips = lax.axis_size(CHIPS)
    samples, features, bag_size = ids.shape
    width = cold_table.shape[1]
    hidden_units, inputs = mlp_weight.shape
    rank = cross_u.shape[1]
    core = lax.axis_index(CORE)

    ids_rows = ids.transpose(2, 1, 0).reshape(bag_size * features, samples)
    send, inverse, position = route(ids_rows, hot_list, location.reshape(-1, 128))
    got = exchange(send.reshape(devices, 1, 128), GRP_DEV).reshape(devices, 128)
    rows = fetch(got, cold_table)
    arrived = exchange(rows.reshape(devices, CAP, width), GRP_DEV).reshape(devices * CAP, width)

    mlp_weight = by_core(mlp_weight)
    mlp_bias = by_core(mlp_bias)
    out_weight = by_core(out_weight)
    hot_rows = hot_table[hot_list[0]]
    hot_index = hot_index.T
    first_input = pool(position, hot_index, hot_rows, arrived)
    cross_low = jnp.dot(first_input, cross_u, preferred_element_type=F32).astype(BF16)
    cross_term = jnp.dot(cross_low, cross_v, preferred_element_type=F32) + cross_bias
    input_wide = first_input.astype(F32)
    cross_out = (input_wide * cross_term + input_wide).astype(BF16)
    hidden_in = contract_cols(cross_out, mlp_weight) + mlp_bias
    hidden = jax.nn.silu(hidden_in).astype(BF16)
    logits = jnp.dot(hidden, out_weight, preferred_element_type=F32)
    logit_grad = jax.nn.sigmoid(logits) - labels.astype(F32)
    out_grad = jnp.dot(logit_grad, hidden.astype(F32), precision=lax.Precision.HIGHEST)
    hidden_grad = (
        logit_grad[:, None] * out_weight.astype(F32)[None, :] * silu_slope(hidden_in)
    ).astype(BF16)
    bias_grad = jnp.sum(hidden_grad.astype(F32), axis=0)

    half = hidden_units // 2
    mine = lax.dynamic_slice(hidden_grad, (0, core * half), (samples, half))
    other = lax.dynamic_slice(hidden_grad, (0, (1 - core) * half), (samples, half))
    other = lax.ppermute(jnp.concatenate([other, cross_out], axis=1), CORE, SWAP)
    mlp_part = contract_rows(
        jnp.concatenate([mine, other[:, :half]], axis=0),
        jnp.concatenate([cross_out, other[:, half:]], axis=0),
    ).astype(BF16)

    cross_out_grad = jnp.dot(hidden_grad, mlp_weight, preferred_element_type=F32)
    term_grad = (cross_out_grad * input_wide).astype(BF16)
    cross_bias_part = jnp.sum(term_grad.astype(F32), axis=0)
    low_grad = contract_cols(term_grad, cross_v).astype(BF16)
    pooled_grad = (
        cross_out_grad * (cross_term + 1.0) + contract_cols(low_grad, cross_u)
    ).astype(BF16)

    mlp_sum = scatter_phase(mlp_part, 0, core).astype(BF16)

    first = core == 0
    pair_u = jnp.concatenate([low_grad, first_input], axis=1)
    pair_v = jnp.concatenate([cross_low, term_grad], axis=1)
    held = jnp.where(first, pair_u, pair_v)
    came = lax.ppermute(jnp.where(first, pair_v, pair_u), CORE, SWAP)
    both = jnp.concatenate([held, came], axis=0)
    cross_part = contract_rows(both[:, :rank], both[:, rank:])
    vectors = jnp.concatenate([cross_bias_part, bias_grad, out_grad])
    vector_rows = vectors.size // 128
    vectors = jnp.pad(
        vectors.reshape(vector_rows, 128), ((0, rank - vector_rows), (0, 4 * WIDE - inputs - 128))
    )
    cross_part = jnp.concatenate(
        [cross_part[:, q * WIDE : (q + 1) * WIDE] for q in range(3)]
        + [jnp.concatenate([cross_part[:, 3 * WIDE :], vectors], axis=1)],
        axis=0,
    ).astype(BF16)
    cross_sum = scatter_phase(cross_part, 0, core).astype(BF16)

    payload = pack(inverse, hot_index, pooled_grad)
    back = exchange(payload, GRP_DEV)

    sums = scatter_phase(jnp.concatenate([mlp_sum, cross_sum], axis=1), 1, core)
    sums = scatter_phase(sums, 2, core)
    mlp_weight_grad = sums[:, :inputs]
    shared = jnp.broadcast_to(sums[None, :, inputs:].astype(BF16), (chips, 16, WIDE))
    shared, back = lax.optimization_barrier((shared, back))
    shared = exchange(shared, CHIPS).reshape(-1, WIDE)
    cold_grad = cold_sum(got, back, cold_table.shape[0])
    hot_grad = hot_sum(got, back, hot_table.shape[0])
    other_shared = lax.ppermute(shared, CORE, SWAP)
    cross_u_grad, cross_v_grad, cross_bias_grad, mlp_bias_grad, out_weight_grad = unpack(
        core, shared, other_shared, inputs, rank, hidden_units
    )
    return (
        cold_grad,
        hot_grad,
        mlp_weight_grad,
        cross_u_grad,
        cross_v_grad,
        cross_bias_grad.reshape(-1),
        mlp_bias_grad.reshape(-1),
        out_weight_grad.reshape(-1),
    )


def solution(mesh):
    torus = Mesh(
        mesh.devices.reshape(mesh.shape["grp"], 4, 4, 2), ("grp", "dev_0", "dev_1", "dev_2")
    )
    placed = (
        P(GRP_DEV, None, None),
        P(),
        P(GRP_DEV, None),
        P(GRP_DEV, None),
        P(GRP_DEV, None),
        P(),
        P(GRP_DEV),
        P(),
        P(),
        P(),
        P(),
        P(),
        P(),
    )
    return jax.shard_map(
        per_device,
        mesh=torus,
        in_specs=placed,
        out_specs=(P(GRP_DEV, None), P(), P(GRP_DEV, None), P(), P(), P(), P(), P()),
        check_vma=False,
    )
```

```python
import jax
import jax.numpy as jnp
from jax import lax
from jax.experimental import pallas as pl
from jax.experimental.pallas import tpu as pltpu
from jax.sharding import Mesh
from jax.sharding import PartitionSpec as P


GRP_DEV = ("grp", "dev_0", "dev_1", "dev_2")
CHIPS = ("grp", "dev_0", "dev_1")
CORE = "dev_2"
SWAP = [(0, 1), (1, 0)]
ORDER = ((2, 1, 0), (0, 2, 1))
CAP = 40
HOT = 32
WIDE = 512
WAYS = 8
F32, BF16, I32 = jnp.float32, jnp.bfloat16, jnp.int32
VMEM = pl.BlockSpec(memory_space=pltpu.VMEM)
SMEM = pl.BlockSpec(memory_space=pltpu.SMEM)


def spread(x, ones):
    return jnp.dot(x.astype(F32).astype(BF16), ones, preferred_element_type=F32).astype(I32)


def route_kernel(ids, hot_list, ids_lanes, location, send, inverse, position, found):
    blocks = position.shape[0]
    features = blocks // 2

    def pick(b, carried):
        for j in range(128):
            found[pl.ds(b * 128 + j, 1), :] = location[pl.ds(ids[b, j] >> 7, 1), :]
        return carried

    lax.fori_loop(0, blocks, pick, 0)
    rows = lax.broadcasted_iota(I32, (128, 128), 0)
    lanes = lax.broadcasted_iota(I32, (128, 128), 1)
    before = (lanes < rows).astype(BF16)
    diagonal = rows == lanes
    ones = jnp.ones((128, 128), BF16)
    low = [
        spread(jnp.where(diagonal, ids_lanes[b : b + 1, :] & 127, 0), ones) for b in range(blocks)
    ]
    value = [
        jnp.where(low[b] == lanes, found[b * 128 : (b + 1) * 128, :], 0) for b in range(blocks)
    ]
    owner = [spread(v >> 11, ones) for v in value]
    high = [spread((v & 2047) >> 4, ones) for v in value]
    deep = [spread(v & 15, ones) for v in value]
    chosen = [o == lanes for o in owner]
    one_hot = [c.astype(F32).astype(BF16) for c in chosen]
    ahead = [jnp.dot(before, o, preferred_element_type=F32) for o in one_hot]
    seen = jnp.zeros((1, 128), F32)
    table = jnp.zeros((128, 256), F32)
    lane_rank = lanes & 63
    left = lanes < 64
    for b in range(blocks):
        rank = spread(jnp.where(chosen[b], ahead[b] + seen, 0.0), ones)
        seen = seen + ahead[b][127:, :] + chosen[b][127:, :].astype(F32)
        hit = lane_rank == rank
        origin = (b % features) * 128 + rows
        slots = jnp.where(hit, jnp.where(left, high[b], deep[b]), 0)
        origins = jnp.where(hit, jnp.where(left, origin >> 4, origin & 15), 0)
        marks = jnp.concatenate(
            [slots.astype(F32).astype(BF16), origins.astype(F32).astype(BF16)], axis=1
        )
        table = table + contract_rows(one_hot[b], marks)
        spot = jnp.where(diagonal, owner[b] * CAP + rank, 0)
        position[b : b + 1, :] = jnp.sum(spot, axis=0, keepdims=True)
    table = table.astype(I32)
    held = spread(jnp.where(diagonal, jnp.broadcast_to(seen, (128, 128)), 0.0), ones)
    wanted = (table[:, :64] << 4) + table[:, 64:128]
    wanted = jnp.where(lanes[:, :64] < held[:, :64], wanted, 2048)
    send[:, :CAP] = wanted[:, :CAP]
    send[:, CAP : CAP + HOT] = jnp.broadcast_to(hot_list[...], (128, HOT))
    send[:, CAP + HOT :] = jnp.zeros((128, 128 - CAP - HOT), I32)
    inverse[...] = (table[:, 128:192] << 4) + table[:, 192:256]


def route(ids, hot_list, location):
    blocks = ids.shape[0]
    return pl.pallas_call(
        route_kernel,
        out_shape=(
            jax.ShapeDtypeStruct((128, 128), I32),
            jax.ShapeDtypeStruct((128, 64), I32),
            jax.ShapeDtypeStruct((blocks, 128), I32),
        ),
        in_specs=[SMEM, VMEM, VMEM, VMEM],
        out_specs=(VMEM, VMEM, VMEM),
        scratch_shapes=[pltpu.VMEM((blocks * 128, 128), I32)],
        name="route",
    )(ids, hot_list, ids, location)


def fetch_kernel(wanted, table, out, wide, picked):
    shard = table.shape[0]
    wide[:shard, :] = table[...].astype(F32)
    wide[shard:, :] = jnp.zeros((8, 128), F32)

    def source(d, carried):
        for i in range(CAP):
            picked[pl.ds(d * CAP + i, 1), :] = wide[pl.ds(wanted[d, i], 1), :]
        return carried

    lax.fori_loop(0, out.shape[0] // CAP, source, 0)
    out[...] = picked[...].astype(BF16)


def fetch(wanted, table):
    count = wanted.shape[0] * CAP
    return pl.pallas_call(
        fetch_kernel,
        out_shape=jax.ShapeDtypeStruct((count, 128), BF16),
        in_specs=[SMEM, VMEM],
        out_specs=VMEM,
        scratch_shapes=[
            pltpu.VMEM((table.shape[0] + 8, 128), F32),
            pltpu.VMEM((count, 128), F32),
        ],
        name="fetch",
    )(wanted, table)


def pool_kernel(position, hot_index, hot_rows, arrived, out, wide, total):
    features, samples = hot_index.shape
    wide[...] = arrived[...].astype(F32)
    slots = lax.broadcasted_iota(I32, (HOT, samples), 0)

    def feature(f, carried):
        for s in range(samples):
            total[s : s + 1, :] = (
                wide[pl.ds(position[f, s], 1), :] + wide[pl.ds(position[features + f, s], 1), :]
            )
        picked = (slots == hot_index[pl.ds(f, 1), :]).astype(F32).astype(BF16)
        both = total[...] + contract_rows(picked, hot_rows[...])
        out[:, pl.ds(pl.multiple_of(f * 128, 128), 128)] = both.astype(BF16)
        return carried

    lax.fori_loop(0, features, feature, 0)


def pool(position, hot_index, hot_rows, arrived):
    features, samples = hot_index.shape
    return pl.pallas_call(
        pool_kernel,
        out_shape=jax.ShapeDtypeStruct((samples, features * 128), BF16),
        in_specs=[SMEM, VMEM, VMEM, VMEM],
        out_specs=VMEM,
        scratch_shapes=[pltpu.VMEM(arrived.shape, F32), pltpu.VMEM((samples, 128), F32)],
        name="pool",
    )(position, hot_index, hot_rows, arrived)


def pack_kernel(inverse, grad, out, wide, picked):
    samples, inputs = grad.shape
    devices = out.shape[0]
    for f in range(inputs // 128):
        part = grad[:, f * 128 : (f + 1) * 128]
        wide[f * samples : (f + 1) * samples, :] = part.astype(F32)

    def source(d, carried):
        for i in range(CAP):
            picked[pl.ds(d * CAP + i, 1), :] = wide[pl.ds(inverse[d, i], 1), :]
        return carried

    lax.fori_loop(0, devices, source, 0)
    out[...] = picked[...].reshape(devices, CAP, 128).astype(BF16)


def pack(inverse, grad):
    devices = inverse.shape[0]
    return pl.pallas_call(
        pack_kernel,
        out_shape=jax.ShapeDtypeStruct((devices, CAP, 128), BF16),
        in_specs=[SMEM, VMEM],
        out_specs=VMEM,
        scratch_shapes=[
            pltpu.VMEM((grad.size // 128, 128), F32),
            pltpu.VMEM((devices * CAP, 128), F32),
        ],
        name="pack",
    )(inverse, grad)


def hot_block_kernel(hot_index, grad, out):
    features, samples = hot_index.shape
    slots = lax.broadcasted_iota(I32, (HOT, samples), 0)
    total = jnp.zeros((HOT, 128), F32)
    for f in range(features):
        one_hot = (slots == hot_index[f : f + 1, :]).astype(F32).astype(BF16)
        part = grad[:, f * 128 : (f + 1) * 128]
        total = total + jnp.dot(one_hot, part, preferred_element_type=F32)
    total = total.astype(BF16)
    for b in range(HOT // 8):
        out[:, b * 128 : (b + 1) * 128] = total[b * 8 : (b + 1) * 8, :]


def hot_block(hot_index, grad):
    return pl.pallas_call(
        hot_block_kernel,
        out_shape=jax.ShapeDtypeStruct((8, HOT // 8 * 128), BF16),
        in_specs=[VMEM, VMEM],
        out_specs=VMEM,
        name="hot_block",
    )(hot_index, grad)


def cold_kernel(wanted, came, out, wide, *sums):
    for way in sums:
        way[...] = jnp.zeros(way.shape, F32)
    wide[...] = came[...].astype(F32)

    def source(d, carried):
        for i in range(CAP // WAYS):
            for k, way in enumerate(sums):
                at = k * (CAP // WAYS) + i
                here = pl.ds(wanted[d, at], 1)
                way[here, :] = way[here, :] + wide[d, at : at + 1, :]
        return carried

    lax.fori_loop(0, wide.shape[0], source, 0)
    shard = out.shape[0]
    total = sums[0][:shard, :]
    for way in sums[1:]:
        total = total + way[:shard, :]
    out[...] = total


def cold_sum(wanted, came, shard_rows):
    return pl.pallas_call(
        cold_kernel,
        out_shape=jax.ShapeDtypeStruct((shard_rows, 128), F32),
        in_specs=[SMEM, VMEM],
        out_specs=VMEM,
        scratch_shapes=[pltpu.VMEM((came.shape[0], CAP, 128), F32)]
        + [pltpu.VMEM((shard_rows + 8, 128), F32)] * WAYS,
        name="cold_sum",
    )(wanted, came)


def hot_kernel(owners, listed, held, came, out, wide_held, wide_came):
    out[...] = jnp.zeros(out.shape, F32)
    tall = held.shape[0]
    for b in range(held.shape[1] // 128):
        lanes = slice(b * 128, (b + 1) * 128)
        wide_held[b * tall : (b + 1) * tall, :] = held[:, lanes].astype(F32)
        wide_came[b * tall : (b + 1) * tall, :] = came[:, lanes].astype(F32)

    def source(k, carried):
        first, second, third = k >> 4, (k >> 2) & 3, k & 3
        base = (second * 8 + (first >> 1) * 2) * tall + third * 16 + (first & 1) * 8
        for side, wide in ((0, wide_held), (1, wide_came)):
            d = owners[side, k]
            places = [pl.ds(listed[d, CAP + i], 1) for i in range(HOT)]
            sums = []
            for i, here in enumerate(places):
                at = (i // 16 * 4 + i // 8 % 2) * tall + i % 8
                sums.append(out[here, :] + wide[pl.ds(base + at, 1), :])
            for here, row in zip(places, sums):
                out[here, :] = row
        return carried

    lax.fori_loop(0, 64, source, 0)


def hot_sum(owners, listed, held, came, hot_rows):
    return pl.pallas_call(
        hot_kernel,
        out_shape=jax.ShapeDtypeStruct((hot_rows, 128), F32),
        in_specs=[SMEM, SMEM, VMEM, VMEM],
        out_specs=VMEM,
        scratch_shapes=[pltpu.VMEM((held.size // 128, 128), F32)] * 2,
        name="hot_sum",
    )(owners, listed, held, came)


def hot_owners(spot, core):
    k = jnp.arange(64, dtype=I32)
    steps = [k >> 4, (k >> 2) & 3, k & 3]
    tables = []
    for c in range(2):
        place = [0, 0, 0]
        for axis, step in zip(ORDER[c], steps):
            back = jnp.where(step == 2, 3, jnp.where(step == 3, 2, step))
            place[axis] = (spot[axis] - back + 4) & 3
        tables.append(((place[0] * 4 + place[1]) * 4 + place[2]) * 2 + c)
    first = core == 0
    return jnp.stack(
        [jnp.where(first, tables[0], tables[1]), jnp.where(first, tables[1], tables[0])]
    )


def unpack_kernel(core, held, came, u_out, v_out, bias_out, mlp_bias_out, out_weight_out, wide):
    first = core[0] == 0
    rank = v_out.shape[0]

    def block(c, chip, lanes):
        here = slice(chip * 16, (chip + 1) * 16)
        own, other = held[here, lanes].astype(F32), came[here, lanes].astype(F32)
        return jnp.where(first, own, other) if c == 0 else jnp.where(first, other, own)

    def chip_of(c, spot):
        place = [0, 0, 0]
        for axis, at in zip(ORDER[c], spot):
            place[axis] = at
        return (place[0] * 4 + place[1]) * 4 + place[2]

    blocks = rank // 16
    for q in range(4):
        count = WIDE if q < 3 else v_out.shape[1] - 3 * WIDE
        for r in range(blocks):
            spot = (q, r // 4, r % 4)
            rows = slice(r * 16, (r + 1) * 16)
            wide[rows, :count] = block(0, chip_of(0, spot), slice(0, count))
            v_out[rows, q * WIDE : q * WIDE + count] = block(1, chip_of(1, spot), slice(0, count))
        u_out[q * WIDE : q * WIDE + count, :] = wide[:, :count].T

    lanes = slice(128, 256)
    sums = jnp.concatenate(
        [
            block(0, chip_of(0, (3, r // 4, r % 4)), lanes)
            + block(1, chip_of(1, (3, r // 4, r % 4)), lanes)
            for r in range(3)
        ]
    )
    bias_out[...] = sums[: bias_out.shape[0]]
    start = bias_out.shape[0]
    for out in (mlp_bias_out, out_weight_out):
        tall = out.shape[0]
        part = sums[start : start + tall]
        start += tall
        for c in range(2):
            for at in range(64):
                spot = (at // 16, at // 4 % 4, at % 4)
                chip = chip_of(c, spot)
                come, go = c * 64 + at, chip * 2 + c
                out[go // 8 : go // 8 + 1, go % 8 * 16 : go % 8 * 16 + 16] = part[
                    come // 8 : come // 8 + 1, come % 8 * 16 : come % 8 * 16 + 16
                ]


def unpack(core, held, came, inputs, rank, hidden_units):
    return pl.pallas_call(
        unpack_kernel,
        out_shape=(
            jax.ShapeDtypeStruct((inputs, rank), F32),
            jax.ShapeDtypeStruct((rank, inputs), F32),
            jax.ShapeDtypeStruct((inputs // 128, 128), F32),
            jax.ShapeDtypeStruct((hidden_units // 128, 128), F32),
            jax.ShapeDtypeStruct((hidden_units // 128, 128), F32),
        ),
        in_specs=[SMEM, VMEM, VMEM],
        out_specs=(VMEM,) * 5,
        scratch_shapes=[pltpu.VMEM((rank, WIDE), F32)],
        name="unpack",
    )(core.reshape(1), held, came)


def silu_slope(values):
    squash = jax.nn.sigmoid(values)
    return squash * (1.0 + values * (1.0 - squash))


def contract_rows(former, latter):
    return lax.dot_general(former, latter, (((0,), (0,)), ((), ())), preferred_element_type=F32)


def contract_cols(former, latter):
    return lax.dot_general(former, latter, (((1,), (1,)), ((), ())), preferred_element_type=F32)


def exchange(x, axes):
    return lax.all_to_all(x, axes, split_axis=0, concat_axis=0, tiled=True)


def route_pairs(phase, shift):
    pairs = []
    for d in range(128):
        spot = [d // 32, d // 8 % 4, d // 2 % 4]
        axis = ORDER[d % 2][phase]
        spot[axis] = (spot[axis] + shift) % 4
        pairs.append((d, ((spot[0] * 4 + spot[1]) * 4 + spot[2]) * 2 + d % 2))
    return pairs


SHIFTS = (1, 3, 2)


def here_of(phase, core):
    here = [lax.axis_index(CHIPS[ORDER[c][phase]]) for c in range(2)]
    return jnp.where(core == 0, here[0], here[1])


def send_on(phase, pieces):
    return [lax.ppermute(p, GRP_DEV, route_pairs(phase, s)) for p, s in zip(pieces, SHIFTS)]


def add_up(own, came):
    total = own.astype(F32)
    for part in came:
        total = total + part.astype(F32)
    return total


def fold_first_kernel(here, mlp, cross, hot, *refs):
    mlp_came, cross_came, (outs, own, hot_out, total) = refs[:3], refs[3:6], (
        refs[6:9],
        refs[9],
        refs[10],
        refs[11],
    )
    tall, inputs = mlp.shape
    part = mlp[...]
    for c in mlp_came:
        part = part + c[...].astype(F32)
    total[:, :inputs] = part
    part = cross[...]
    for c in cross_came:
        part = part + c[:tall, :].astype(F32)
    total[:, inputs:] = part
    blocks = [hot[...].astype(F32)] + [c[tall:, :].astype(F32) for c in cross_came]
    lanes = hot.shape[1] // 2
    hot_rows = jnp.concatenate(
        [b[:, :lanes] for b in blocks] + [b[:, lanes:] for b in blocks]
    ).astype(BF16)
    hot_out[...] = hot_rows
    count = tall // 4
    for out, s in zip(outs, SHIFTS):
        at = pl.multiple_of(((here[0] + s) & 3) * count, count)
        out[:, : total.shape[1]] = total[pl.ds(at, count), :].astype(BF16)
        out[:, total.shape[1] :] = hot_rows
    own[...] = total[pl.ds(pl.multiple_of(here[0] * count, count), count), :]


def fold_first(here, mlp, cross, hot, mlp_came, cross_came):
    tall, wide = mlp.shape[0], mlp.shape[1] + cross.shape[1]
    lanes = hot.shape[1] // 2
    out = jax.ShapeDtypeStruct((tall // 4, wide + lanes), BF16)
    got = pl.pallas_call(
        fold_first_kernel,
        out_shape=(out, out, out)
        + (
            jax.ShapeDtypeStruct((tall // 4, wide), F32),
            jax.ShapeDtypeStruct((tall // 4, lanes), BF16),
        ),
        in_specs=[SMEM] + [VMEM] * 9,
        out_specs=(VMEM,) * 5,
        scratch_shapes=[pltpu.VMEM((tall, wide), F32)],
        name="fold_first",
    )(here.reshape(1), mlp, cross, hot, *mlp_came, *cross_came)
    return got[:3], got[3], got[4]


def fold_second_kernel(here, own_in, hot, *refs):
    came, outs, own, hot_out, total = refs[:3], refs[3:6], refs[6], refs[7], refs[8]
    wide = own_in.shape[1]
    lanes = hot.shape[1]
    part = own_in[...]
    for c in came:
        part = part + c[:, :wide].astype(F32)
    total[...] = part
    blocks = [hot[...]] + [c[:, wide:] for c in came]
    for j, block in enumerate(blocks):
        for t in range(4):
            hot_out[:, (j * 4 + t) * lanes : (j * 4 + t + 1) * lanes] = block[t * 16 : t * 16 + 16]
    for out, s in zip(outs, SHIFTS):
        at = pl.multiple_of(((here[0] + s) & 3) * 16, 16)
        out[:, :wide] = total[pl.ds(at, 16), :].astype(BF16)
        out[:, wide:] = hot_out[...]
    own[...] = total[pl.ds(pl.multiple_of(here[0] * 16, 16), 16), :]


def fold_second(here, own, hot, came):
    wide, lanes = own.shape[1], 16 * hot.shape[1]
    out = jax.ShapeDtypeStruct((16, wide + lanes), BF16)
    got = pl.pallas_call(
        fold_second_kernel,
        out_shape=(out, out, out)
        + (jax.ShapeDtypeStruct((16, wide), F32), jax.ShapeDtypeStruct((16, lanes), BF16)),
        in_specs=[SMEM] + [VMEM] * 5,
        out_specs=(VMEM,) * 5,
        scratch_shapes=[pltpu.VMEM(own.shape, F32)],
        name="fold_second",
    )(here.reshape(1), own, hot, *came)
    return got[:3], got[3], got[4]


def by_core(x):
    parts = x.reshape(4, 4, 4, 2, 16, *x.shape[1:])
    halves = []
    for c in range(2):
        rest = tuple(range(3, 3 + x.ndim))
        half = parts[:, :, :, c].transpose(*ORDER[c], *rest)
        halves.append(half.reshape(-1, *x.shape[1:]))
    return jnp.concatenate(halves)


def per_device(
    ids,
    location,
    cold_table,
    hot_index,
    hot_list,
    hot_table,
    labels,
    cross_u,
    cross_v,
    cross_bias,
    mlp_weight,
    mlp_bias,
    out_weight,
):
    devices = lax.axis_size(GRP_DEV)
    chips = lax.axis_size(CHIPS)
    samples, features, bag_size = ids.shape
    width = cold_table.shape[1]
    hidden_units, inputs = mlp_weight.shape
    rank = cross_u.shape[1]
    core = lax.axis_index(CORE)

    ids_rows = ids.transpose(2, 1, 0).reshape(bag_size * features, samples)
    send, inverse, position = route(ids_rows, hot_list, location.reshape(-1, 128))
    got = exchange(send.reshape(devices, 1, 128), GRP_DEV).reshape(devices, 128)
    rows = fetch(got, cold_table)
    arrived = exchange(rows.reshape(devices, CAP, width), GRP_DEV).reshape(devices * CAP, width)

    mlp_weight = by_core(mlp_weight)
    mlp_bias = by_core(mlp_bias)
    out_weight = by_core(out_weight)
    hot_rows = hot_table[hot_list[0]]
    hot_index = hot_index.T
    first_input = pool(position, hot_index, hot_rows, arrived)
    cross_low = jnp.dot(first_input, cross_u, preferred_element_type=F32).astype(BF16)
    cross_term = jnp.dot(cross_low, cross_v, preferred_element_type=F32) + cross_bias
    input_wide = first_input.astype(F32)
    cross_out = (input_wide * cross_term + input_wide).astype(BF16)
    hidden_in = contract_cols(cross_out, mlp_weight) + mlp_bias
    hidden = jax.nn.silu(hidden_in).astype(BF16)
    logits = jnp.dot(hidden, out_weight, preferred_element_type=F32)
    logit_grad = jax.nn.sigmoid(logits) - labels.astype(F32)
    out_grad = jnp.dot(logit_grad, hidden.astype(F32), precision=lax.Precision.HIGHEST)
    hidden_grad = (
        logit_grad[:, None] * out_weight.astype(F32)[None, :] * silu_slope(hidden_in)
    ).astype(BF16)
    bias_grad = jnp.sum(hidden_grad.astype(F32), axis=0)

    half = hidden_units // 2
    mine = lax.dynamic_slice(hidden_grad, (0, core * half), (samples, half))
    other = lax.dynamic_slice(hidden_grad, (0, (1 - core) * half), (samples, half))
    other = lax.ppermute(jnp.concatenate([other, cross_out], axis=1), CORE, SWAP)
    left = jnp.concatenate([mine, other[:, :half]], axis=0)
    right = jnp.concatenate([cross_out, other[:, half:]], axis=0)
    here = here_of(0, core)

    def mlp_piece(shift):
        at = (here + shift) % 4 * (half // 4)
        return contract_rows(lax.dynamic_slice_in_dim(left, at, half // 4, 1), right)

    cross_out_grad = jnp.dot(hidden_grad, mlp_weight, preferred_element_type=F32)
    term_grad = (cross_out_grad * input_wide).astype(BF16)
    cross_bias_part = jnp.sum(term_grad.astype(F32), axis=0)
    low_grad = contract_cols(term_grad, cross_v).astype(BF16)
    pooled_grad = (
        cross_out_grad * (cross_term + 1.0) + contract_cols(low_grad, cross_u)
    ).astype(BF16)

    mlp_came = send_on(0, [mlp_piece(s).astype(BF16) for s in SHIFTS])

    first = core == 0
    pad = jnp.zeros((samples, 4 * WIDE - inputs), BF16)
    pair_u = jnp.concatenate([low_grad, first_input, pad], axis=1)
    pair_v = jnp.concatenate([cross_low, term_grad, pad], axis=1)
    held = jnp.where(first, pair_u, pair_v)
    came = lax.ppermute(jnp.where(first, pair_v, pair_u), CORE, SWAP)
    both = jnp.concatenate([held, came], axis=0)
    vectors = jnp.concatenate([cross_bias_part, bias_grad, out_grad])
    vector_rows = vectors.size // 128
    start = inputs - 3 * WIDE
    vectors = jnp.pad(
        vectors.reshape(vector_rows, 128), ((0, rank - vector_rows), (start, WIDE - start - 128))
    )

    def cross_piece(shift):
        at = (here + shift) % 4
        part = lax.dynamic_slice_in_dim(both, rank + at * WIDE, WIDE, 1)
        return contract_rows(both[:, :rank], part) + jnp.where(at == 3, vectors, 0.0)

    hot_part = hot_block(hot_index, pooled_grad)
    cross_came = send_on(
        0, [jnp.concatenate([cross_piece(s).astype(BF16), hot_part]) for s in SHIFTS]
    )

    payload = pack(inverse, pooled_grad)
    back = exchange(payload, GRP_DEV)

    pieces, own, hot_part = fold_first(
        here_of(1, core), mlp_piece(0), cross_piece(0), hot_part, mlp_came, cross_came
    )
    came = send_on(1, pieces)
    pieces, own, hot_part = fold_second(here_of(2, core), own, hot_part, came)
    came = send_on(2, pieces)
    wide = own.shape[1]
    sums = add_up(own, [c[:, :wide] for c in came])
    hot_part = jnp.concatenate([hot_part] + [c[:, wide:] for c in came])
    mlp_weight_grad = sums[:, :inputs]
    shared = jnp.broadcast_to(sums[None, :, inputs:].astype(BF16), (chips, 16, WIDE))
    shared, back = lax.optimization_barrier((shared, back))
    shared = exchange(shared, CHIPS).reshape(-1, WIDE)
    hot_other = lax.ppermute(hot_part, CORE, SWAP)
    cold_grad = cold_sum(got, back, cold_table.shape[0])
    owners = hot_owners([lax.axis_index(axis) for axis in CHIPS], core)
    hot_grad = hot_sum(owners, got, hot_part, hot_other, hot_table.shape[0])
    other_shared = lax.ppermute(shared, CORE, SWAP)
    cross_u_grad, cross_v_grad, cross_bias_grad, mlp_bias_grad, out_weight_grad = unpack(
        core, shared, other_shared, inputs, rank, hidden_units
    )
    return (
        cold_grad,
        hot_grad,
        mlp_weight_grad,
        cross_u_grad,
        cross_v_grad,
        cross_bias_grad.reshape(-1),
        mlp_bias_grad.reshape(-1),
        out_weight_grad.reshape(-1),
    )


def solution(mesh):
    torus = Mesh(
        mesh.devices.reshape(mesh.shape["grp"], 4, 4, 2), ("grp", "dev_0", "dev_1", "dev_2")
    )
    placed = (
        P(GRP_DEV, None, None),
        P(),
        P(GRP_DEV, None),
        P(GRP_DEV, None),
        P(GRP_DEV, None),
        P(),
        P(GRP_DEV),
        P(),
        P(),
        P(),
        P(),
        P(),
        P(),
    )
    return jax.shard_map(
        per_device,
        mesh=torus,
        in_specs=placed,
        out_specs=(P(GRP_DEV, None), P(), P(GRP_DEV, None), P(), P(), P(), P(), P()),
        check_vma=False,
    )
```

```python
import jax
import jax.numpy as jnp
from jax import lax
from jax.experimental import pallas as pl
from jax.experimental.pallas import tpu as pltpu
from jax.sharding import Mesh
from jax.sharding import PartitionSpec as P


GRP_DEV = ("grp", "dev_0", "dev_1", "dev_2")
CHIPS = ("grp", "dev_0", "dev_1")
CORE = "dev_2"
SWAP = [(0, 1), (1, 0)]
ORDER = ((2, 1, 0), (0, 2, 1))
CAP = 40
HOT = 32
WIDE = 512
WAYS = 8
F32, BF16, I32 = jnp.float32, jnp.bfloat16, jnp.int32
VMEM = pl.BlockSpec(memory_space=pltpu.VMEM)
SMEM = pl.BlockSpec(memory_space=pltpu.SMEM)


def spread(x, ones):
    return jnp.dot(x.astype(F32).astype(BF16), ones, preferred_element_type=F32).astype(I32)


def route_kernel(ids, hot_list, ids_lanes, location, send, inverse, position, found):
    blocks = position.shape[0]
    features = blocks // 2

    def pick(b, carried):
        for j in range(128):
            found[pl.ds(b * 128 + j, 1), :] = location[pl.ds(ids[b, j] >> 7, 1), :]
        return carried

    lax.fori_loop(0, blocks, pick, 0)
    rows = lax.broadcasted_iota(I32, (128, 128), 0)
    lanes = lax.broadcasted_iota(I32, (128, 128), 1)
    before = (lanes < rows).astype(BF16)
    diagonal = rows == lanes
    ones = jnp.ones((128, 128), BF16)
    low = [
        spread(jnp.where(diagonal, ids_lanes[b : b + 1, :] & 127, 0), ones) for b in range(blocks)
    ]
    value = [
        jnp.where(low[b] == lanes, found[b * 128 : (b + 1) * 128, :], 0) for b in range(blocks)
    ]
    owner = [spread(v >> 11, ones) for v in value]
    high = [spread((v & 2047) >> 4, ones) for v in value]
    deep = [spread(v & 15, ones) for v in value]
    chosen = [o == lanes for o in owner]
    one_hot = [c.astype(F32).astype(BF16) for c in chosen]
    ahead = [jnp.dot(before, o, preferred_element_type=F32) for o in one_hot]
    seen = jnp.zeros((1, 128), F32)
    table = jnp.zeros((128, 256), F32)
    lane_rank = lanes & 63
    left = lanes < 64
    for b in range(blocks):
        rank = spread(jnp.where(chosen[b], ahead[b] + seen, 0.0), ones)
        seen = seen + ahead[b][127:, :] + chosen[b][127:, :].astype(F32)
        hit = lane_rank == rank
        origin = (b % features) * 128 + rows
        slots = jnp.where(hit, jnp.where(left, high[b], deep[b]), 0)
        origins = jnp.where(hit, jnp.where(left, origin >> 4, origin & 15), 0)
        marks = jnp.concatenate(
            [slots.astype(F32).astype(BF16), origins.astype(F32).astype(BF16)], axis=1
        )
        table = table + contract_rows(one_hot[b], marks)
        spot = jnp.where(diagonal, owner[b] * CAP + rank, 0)
        position[b : b + 1, :] = jnp.sum(spot, axis=0, keepdims=True)
    table = table.astype(I32)
    held = spread(jnp.where(diagonal, jnp.broadcast_to(seen, (128, 128)), 0.0), ones)
    wanted = (table[:, :64] << 4) + table[:, 64:128]
    wanted = jnp.where(lanes[:, :64] < held[:, :64], wanted, 2048)
    send[:, :CAP] = wanted[:, :CAP]
    send[:, CAP : CAP + HOT] = jnp.broadcast_to(hot_list[...], (128, HOT))
    send[:, CAP + HOT :] = jnp.zeros((128, 128 - CAP - HOT), I32)
    inverse[...] = (table[:, 128:192] << 4) + table[:, 192:256]


def route(ids, hot_list, location):
    blocks = ids.shape[0]
    return pl.pallas_call(
        route_kernel,
        out_shape=(
            jax.ShapeDtypeStruct((128, 128), I32),
            jax.ShapeDtypeStruct((128, 64), I32),
            jax.ShapeDtypeStruct((blocks, 128), I32),
        ),
        in_specs=[SMEM, VMEM, VMEM, VMEM],
        out_specs=(VMEM, VMEM, VMEM),
        scratch_shapes=[pltpu.VMEM((blocks * 128, 128), I32)],
        name="route",
    )(ids, hot_list, ids, location)


def fetch_kernel(wanted, table, out, wide, picked):
    shard = table.shape[0]
    wide[:shard, :] = table[...].astype(F32)
    wide[shard:, :] = jnp.zeros((8, 128), F32)

    def source(d, carried):
        for i in range(CAP):
            picked[pl.ds(d * CAP + i, 1), :] = wide[pl.ds(wanted[d, i], 1), :]
        return carried

    lax.fori_loop(0, out.shape[0] // CAP, source, 0)
    out[...] = picked[...].astype(BF16)


def fetch(wanted, table):
    count = wanted.shape[0] * CAP
    return pl.pallas_call(
        fetch_kernel,
        out_shape=jax.ShapeDtypeStruct((count, 128), BF16),
        in_specs=[SMEM, VMEM],
        out_specs=VMEM,
        scratch_shapes=[
            pltpu.VMEM((table.shape[0] + 8, 128), F32),
            pltpu.VMEM((count, 128), F32),
        ],
        name="fetch",
    )(wanted, table)


def pool_kernel(position, hot_index, hot_rows, arrived, out, wide, total):
    features, samples = hot_index.shape
    wide[...] = arrived[...].astype(F32)
    slots = lax.broadcasted_iota(I32, (HOT, samples), 0)

    def feature(f, carried):
        for s in range(samples):
            total[s : s + 1, :] = (
                wide[pl.ds(position[f, s], 1), :] + wide[pl.ds(position[features + f, s], 1), :]
            )
        picked = (slots == hot_index[pl.ds(f, 1), :]).astype(F32).astype(BF16)
        both = total[...] + contract_rows(picked, hot_rows[...])
        out[:, pl.ds(pl.multiple_of(f * 128, 128), 128)] = both.astype(BF16)
        return carried

    lax.fori_loop(0, features, feature, 0)


def pool(position, hot_index, hot_rows, arrived):
    features, samples = hot_index.shape
    return pl.pallas_call(
        pool_kernel,
        out_shape=jax.ShapeDtypeStruct((samples, features * 128), BF16),
        in_specs=[SMEM, VMEM, VMEM, VMEM],
        out_specs=VMEM,
        scratch_shapes=[pltpu.VMEM(arrived.shape, F32), pltpu.VMEM((samples, 128), F32)],
        name="pool",
    )(position, hot_index, hot_rows, arrived)


def pack_kernel(inverse, grad, out, wide, picked):
    samples, inputs = grad.shape
    devices = out.shape[0]
    for f in range(inputs // 128):
        part = grad[:, f * 128 : (f + 1) * 128]
        wide[f * samples : (f + 1) * samples, :] = part.astype(F32)

    def source(d, carried):
        for i in range(CAP):
            picked[pl.ds(d * CAP + i, 1), :] = wide[pl.ds(inverse[d, i], 1), :]
        return carried

    lax.fori_loop(0, devices, source, 0)
    out[...] = picked[...].reshape(devices, CAP, 128).astype(BF16)


def pack(inverse, grad):
    devices = inverse.shape[0]
    return pl.pallas_call(
        pack_kernel,
        out_shape=jax.ShapeDtypeStruct((devices, CAP, 128), BF16),
        in_specs=[SMEM, VMEM],
        out_specs=VMEM,
        scratch_shapes=[
            pltpu.VMEM((grad.size // 128, 128), F32),
            pltpu.VMEM((devices * CAP, 128), F32),
        ],
        name="pack",
    )(inverse, grad)


def hot_block_kernel(hot_index, grad, out):
    features, samples = hot_index.shape
    slots = lax.broadcasted_iota(I32, (HOT, samples), 0)
    total = jnp.zeros((HOT, 128), F32)
    for f in range(features):
        one_hot = (slots == hot_index[f : f + 1, :]).astype(F32).astype(BF16)
        part = grad[:, f * 128 : (f + 1) * 128]
        total = total + jnp.dot(one_hot, part, preferred_element_type=F32)
    total = total.astype(BF16)
    for b in range(HOT // 8):
        out[:, b * 128 : (b + 1) * 128] = total[b * 8 : (b + 1) * 8, :]


def hot_block(hot_index, grad):
    return pl.pallas_call(
        hot_block_kernel,
        out_shape=jax.ShapeDtypeStruct((8, HOT // 8 * 128), BF16),
        in_specs=[VMEM, VMEM],
        out_specs=VMEM,
        name="hot_block",
    )(hot_index, grad)


def cold_kernel(wanted, came, out, wide, *sums):
    for way in sums:
        way[...] = jnp.zeros(way.shape, F32)
    wide[...] = came[...].astype(F32)

    def source(d, carried):
        for i in range(CAP // WAYS):
            for k, way in enumerate(sums):
                at = k * (CAP // WAYS) + i
                here = pl.ds(wanted[d, at], 1)
                way[here, :] = way[here, :] + wide[d, at : at + 1, :]
        return carried

    lax.fori_loop(0, wide.shape[0], source, 0)
    shard = out.shape[0]
    total = sums[0][:shard, :]
    for way in sums[1:]:
        total = total + way[:shard, :]
    out[...] = total


def cold_sum(wanted, came, shard_rows):
    return pl.pallas_call(
        cold_kernel,
        out_shape=jax.ShapeDtypeStruct((shard_rows, 128), F32),
        in_specs=[SMEM, VMEM],
        out_specs=VMEM,
        scratch_shapes=[pltpu.VMEM((came.shape[0], CAP, 128), F32)]
        + [pltpu.VMEM((shard_rows + 8, 128), F32)] * WAYS,
        name="cold_sum",
    )(wanted, came)


def hot_kernel(owners, listed, held, came, out, wide_held, wide_came):
    out[...] = jnp.zeros(out.shape, F32)
    tall = held.shape[0]
    for b in range(held.shape[1] // 128):
        lanes = slice(b * 128, (b + 1) * 128)
        wide_held[b * tall : (b + 1) * tall, :] = held[:, lanes].astype(F32)
        wide_came[b * tall : (b + 1) * tall, :] = came[:, lanes].astype(F32)

    def source(k, carried):
        first, second, third = k >> 4, (k >> 2) & 3, k & 3
        base = (second * 8 + (first >> 1) * 2) * tall + third * 16 + (first & 1) * 8
        for side, wide in ((0, wide_held), (1, wide_came)):
            d = owners[side, k]
            places = [pl.ds(listed[d, CAP + i], 1) for i in range(HOT)]
            sums = []
            for i, here in enumerate(places):
                at = (i // 16 * 4 + i // 8 % 2) * tall + i % 8
                sums.append(out[here, :] + wide[pl.ds(base + at, 1), :])
            for here, row in zip(places, sums):
                out[here, :] = row
        return carried

    lax.fori_loop(0, 64, source, 0)


def hot_sum(owners, listed, held, came, hot_rows):
    return pl.pallas_call(
        hot_kernel,
        out_shape=jax.ShapeDtypeStruct((hot_rows, 128), F32),
        in_specs=[SMEM, SMEM, VMEM, VMEM],
        out_specs=VMEM,
        scratch_shapes=[pltpu.VMEM((held.size // 128, 128), F32)] * 2,
        name="hot_sum",
    )(owners, listed, held, came)


def hot_owners(spot, core):
    k = jnp.arange(64, dtype=I32)
    steps = [k >> 4, (k >> 2) & 3, k & 3]
    tables = []
    for c in range(2):
        place = [0, 0, 0]
        for axis, step in zip(ORDER[c], steps):
            back = jnp.where(step == 2, 3, jnp.where(step == 3, 2, step))
            place[axis] = (spot[axis] - back + 4) & 3
        tables.append(((place[0] * 4 + place[1]) * 4 + place[2]) * 2 + c)
    first = core == 0
    return jnp.stack(
        [jnp.where(first, tables[0], tables[1]), jnp.where(first, tables[1], tables[0])]
    )


def unpack_kernel(core, held, came, u_out, v_out, bias_out, mlp_bias_out, out_weight_out, wide):
    first = core[0] == 0
    rank = v_out.shape[0]

    def block(c, chip, lanes):
        here = slice(chip * 16, (chip + 1) * 16)
        own, other = held[here, lanes].astype(F32), came[here, lanes].astype(F32)
        return jnp.where(first, own, other) if c == 0 else jnp.where(first, other, own)

    def chip_of(c, spot):
        place = [0, 0, 0]
        for axis, at in zip(ORDER[c], spot):
            place[axis] = at
        return (place[0] * 4 + place[1]) * 4 + place[2]

    blocks = rank // 16
    for q in range(4):
        count = WIDE if q < 3 else v_out.shape[1] - 3 * WIDE
        for r in range(blocks):
            spot = (q, r // 4, r % 4)
            rows = slice(r * 16, (r + 1) * 16)
            wide[rows, :count] = block(0, chip_of(0, spot), slice(0, count))
            v_out[rows, q * WIDE : q * WIDE + count] = block(1, chip_of(1, spot), slice(0, count))
        u_out[q * WIDE : q * WIDE + count, :] = wide[:, :count].T

    lanes = slice(128, 256)
    sums = jnp.concatenate(
        [
            block(0, chip_of(0, (3, r // 4, r % 4)), lanes)
            + block(1, chip_of(1, (3, r // 4, r % 4)), lanes)
            for r in range(3)
        ]
    )
    bias_out[...] = sums[: bias_out.shape[0]]
    start = bias_out.shape[0]
    for out in (mlp_bias_out, out_weight_out):
        tall = out.shape[0]
        part = sums[start : start + tall]
        start += tall
        for c in range(2):
            for at in range(64):
                spot = (at // 16, at // 4 % 4, at % 4)
                chip = chip_of(c, spot)
                come, go = c * 64 + at, chip * 2 + c
                out[go // 8 : go // 8 + 1, go % 8 * 16 : go % 8 * 16 + 16] = part[
                    come // 8 : come // 8 + 1, come % 8 * 16 : come % 8 * 16 + 16
                ]


def unpack(core, held, came, inputs, rank, hidden_units):
    return pl.pallas_call(
        unpack_kernel,
        out_shape=(
            jax.ShapeDtypeStruct((inputs, rank), F32),
            jax.ShapeDtypeStruct((rank, inputs), F32),
            jax.ShapeDtypeStruct((inputs // 128, 128), F32),
            jax.ShapeDtypeStruct((hidden_units // 128, 128), F32),
            jax.ShapeDtypeStruct((hidden_units // 128, 128), F32),
        ),
        in_specs=[SMEM, VMEM, VMEM],
        out_specs=(VMEM,) * 5,
        scratch_shapes=[pltpu.VMEM((rank, WIDE), F32)],
        name="unpack",
    )(core.reshape(1), held, came)


def silu_slope(values):
    squash = jax.nn.sigmoid(values)
    return squash * (1.0 + values * (1.0 - squash))


def contract_rows(former, latter):
    return lax.dot_general(former, latter, (((0,), (0,)), ((), ())), preferred_element_type=F32)


def contract_cols(former, latter):
    return lax.dot_general(former, latter, (((1,), (1,)), ((), ())), preferred_element_type=F32)


def exchange(x, axes):
    return lax.all_to_all(x, axes, split_axis=0, concat_axis=0, tiled=True)


def route_pairs(phase, shift):
    pairs = []
    for d in range(128):
        spot = [d // 32, d // 8 % 4, d // 2 % 4]
        axis = ORDER[d % 2][phase]
        spot[axis] = (spot[axis] + shift) % 4
        pairs.append((d, ((spot[0] * 4 + spot[1]) * 4 + spot[2]) * 2 + d % 2))
    return pairs


SHIFTS = (1, 3, 2)


def here_of(phase, core):
    here = [lax.axis_index(CHIPS[ORDER[c][phase]]) for c in range(2)]
    return jnp.where(core == 0, here[0], here[1])


def send_on(phase, pieces):
    return [lax.ppermute(p, GRP_DEV, route_pairs(phase, s)) for p, s in zip(pieces, SHIFTS)]


def add_up(own, came):
    total = own.astype(F32)
    for part in came:
        total = total + part.astype(F32)
    return total


def fold_first_kernel(here, mlp, cross, hot, *refs):
    mlp_came, cross_came, (outs, own, hot_out, total) = refs[:3], refs[3:6], (
        refs[6:9],
        refs[9],
        refs[10],
        refs[11],
    )
    tall, inputs = mlp.shape
    part = mlp[...]
    for c in mlp_came:
        part = part + c[...].astype(F32)
    total[:, :inputs] = part
    part = cross[...]
    for c in cross_came:
        part = part + c[:tall, :].astype(F32)
    total[:, inputs:] = part
    blocks = [hot[...].astype(F32)] + [c[tall:, :].astype(F32) for c in cross_came]
    lanes = hot.shape[1] // 2
    hot_rows = jnp.concatenate(
        [b[:, :lanes] for b in blocks] + [b[:, lanes:] for b in blocks]
    ).astype(BF16)
    hot_out[...] = hot_rows
    count = tall // 4
    for out, s in zip(outs, SHIFTS):
        at = pl.multiple_of(((here[0] + s) & 3) * count, count)
        out[:, : total.shape[1]] = total[pl.ds(at, count), :].astype(BF16)
        out[:, total.shape[1] :] = hot_rows
    own[...] = total[pl.ds(pl.multiple_of(here[0] * count, count), count), :]


def fold_first(here, mlp, cross, hot, mlp_came, cross_came):
    tall, wide = mlp.shape[0], mlp.shape[1] + cross.shape[1]
    lanes = hot.shape[1] // 2
    out = jax.ShapeDtypeStruct((tall // 4, wide + lanes), BF16)
    got = pl.pallas_call(
        fold_first_kernel,
        out_shape=(out, out, out)
        + (
            jax.ShapeDtypeStruct((tall // 4, wide), F32),
            jax.ShapeDtypeStruct((tall // 4, lanes), BF16),
        ),
        in_specs=[SMEM] + [VMEM] * 9,
        out_specs=(VMEM,) * 5,
        scratch_shapes=[pltpu.VMEM((tall, wide), F32)],
        name="fold_first",
    )(here.reshape(1), mlp, cross, hot, *mlp_came, *cross_came)
    return got[:3], got[3], got[4]


def fold_second_kernel(here, own_in, hot, *refs):
    came, outs, own, hot_out, total = refs[:3], refs[3:6], refs[6], refs[7], refs[8]
    wide = own_in.shape[1]
    lanes = hot.shape[1]
    part = own_in[...]
    for c in came:
        part = part + c[:, :wide].astype(F32)
    total[...] = part
    blocks = [hot[...]] + [c[:, wide:] for c in came]
    for j, block in enumerate(blocks):
        for t in range(4):
            hot_out[:, (j * 4 + t) * lanes : (j * 4 + t + 1) * lanes] = block[t * 16 : t * 16 + 16]
    for out, s in zip(outs, SHIFTS):
        at = pl.multiple_of(((here[0] + s) & 3) * 16, 16)
        out[:, :wide] = total[pl.ds(at, 16), :].astype(BF16)
        out[:, wide:] = hot_out[...]
    own[...] = total[pl.ds(pl.multiple_of(here[0] * 16, 16), 16), :]


def fold_second(here, own, hot, came):
    wide, lanes = own.shape[1], 16 * hot.shape[1]
    out = jax.ShapeDtypeStruct((16, wide + lanes), BF16)
    got = pl.pallas_call(
        fold_second_kernel,
        out_shape=(out, out, out)
        + (jax.ShapeDtypeStruct((16, wide), F32), jax.ShapeDtypeStruct((16, lanes), BF16)),
        in_specs=[SMEM] + [VMEM] * 5,
        out_specs=(VMEM,) * 5,
        scratch_shapes=[pltpu.VMEM(own.shape, F32)],
        name="fold_second",
    )(here.reshape(1), own, hot, *came)
    return got[:3], got[3], got[4]


def by_core(x):
    parts = x.reshape(4, 4, 4, 2, 16, *x.shape[1:])
    halves = []
    for c in range(2):
        rest = tuple(range(3, 3 + x.ndim))
        half = parts[:, :, :, c].transpose(*ORDER[c], *rest)
        halves.append(half.reshape(-1, *x.shape[1:]))
    return jnp.concatenate(halves)


def per_device(
    ids,
    location,
    cold_table,
    hot_index,
    hot_list,
    hot_table,
    labels,
    cross_u,
    cross_v,
    cross_bias,
    mlp_weight,
    mlp_bias,
    out_weight,
):
    devices = lax.axis_size(GRP_DEV)
    chips = lax.axis_size(CHIPS)
    samples, features, bag_size = ids.shape
    width = cold_table.shape[1]
    hidden_units, inputs = mlp_weight.shape
    rank = cross_u.shape[1]
    core = lax.axis_index(CORE)

    ids_rows = ids.transpose(2, 1, 0).reshape(bag_size * features, samples)
    send, inverse, position = route(ids_rows, hot_list, location.reshape(-1, 128))
    got = exchange(send.reshape(devices, 1, 128), GRP_DEV).reshape(devices, 128)
    rows = fetch(got, cold_table)
    arrived = exchange(rows.reshape(devices, CAP, width), GRP_DEV).reshape(devices * CAP, width)

    mlp_weight = by_core(mlp_weight)
    mlp_bias = by_core(mlp_bias)
    out_weight = by_core(out_weight)
    hot_rows = hot_table[hot_list[0]]
    hot_index = hot_index.T
    first_input = pool(position, hot_index, hot_rows, arrived)
    cross_low = jnp.dot(first_input, cross_u, preferred_element_type=F32).astype(BF16)
    cross_term = jnp.dot(cross_low, cross_v, preferred_element_type=F32) + cross_bias
    input_wide = first_input.astype(F32)
    cross_out = (input_wide * cross_term + input_wide).astype(BF16)
    hidden_in = contract_cols(cross_out, mlp_weight) + mlp_bias
    hidden = jax.nn.silu(hidden_in).astype(BF16)
    logits = jnp.dot(hidden, out_weight, preferred_element_type=F32)
    logit_grad = jax.nn.sigmoid(logits) - labels.astype(F32)
    out_grad = jnp.dot(logit_grad, hidden.astype(F32), precision=lax.Precision.HIGHEST)
    hidden_grad = (
        logit_grad[:, None] * out_weight.astype(F32)[None, :] * silu_slope(hidden_in)
    ).astype(BF16)
    bias_grad = jnp.sum(hidden_grad.astype(F32), axis=0)

    half = hidden_units // 2
    mine = lax.dynamic_slice(hidden_grad, (0, core * half), (samples, half))
    other = lax.dynamic_slice(hidden_grad, (0, (1 - core) * half), (samples, half))
    other = lax.ppermute(jnp.concatenate([other, cross_out], axis=1), CORE, SWAP)
    left = jnp.concatenate([mine, other[:, :half]], axis=0)
    right = jnp.concatenate([cross_out, other[:, half:]], axis=0)
    here = here_of(0, core)

    def mlp_piece(shift):
        at = (here + shift) % 4 * (half // 4)
        return contract_rows(lax.dynamic_slice_in_dim(left, at, half // 4, 1), right)

    cross_out_grad = jnp.dot(hidden_grad, mlp_weight, preferred_element_type=F32)
    term_grad = (cross_out_grad * input_wide).astype(BF16)
    cross_bias_part = jnp.sum(term_grad.astype(F32), axis=0)
    low_grad = contract_cols(term_grad, cross_v).astype(BF16)
    pooled_grad = (
        cross_out_grad * (cross_term + 1.0) + contract_cols(low_grad, cross_u)
    ).astype(BF16)

    mlp_came = send_on(0, [mlp_piece(s).astype(BF16) for s in SHIFTS])

    first = core == 0
    pad = jnp.zeros((samples, 4 * WIDE - inputs), BF16)
    pair_u = jnp.concatenate([low_grad, first_input, pad], axis=1)
    pair_v = jnp.concatenate([cross_low, term_grad, pad], axis=1)
    held = jnp.where(first, pair_u, pair_v)
    came = lax.ppermute(jnp.where(first, pair_v, pair_u), CORE, SWAP)
    both = jnp.concatenate([held, came], axis=0)
    vectors = jnp.concatenate([cross_bias_part, bias_grad, out_grad])
    vector_rows = vectors.size // 128
    start = inputs - 3 * WIDE
    vectors = jnp.pad(
        vectors.reshape(vector_rows, 128), ((0, rank - vector_rows), (start, WIDE - start - 128))
    )

    def cross_piece(shift):
        at = (here + shift) % 4
        part = lax.dynamic_slice_in_dim(both, rank + at * WIDE, WIDE, 1)
        return contract_rows(both[:, :rank], part) + jnp.where(at == 3, vectors, 0.0)

    hot_part = hot_block(hot_index, pooled_grad)
    cross_came = send_on(
        0, [jnp.concatenate([cross_piece(s).astype(BF16), hot_part]) for s in SHIFTS]
    )

    payload = pack(inverse, pooled_grad)
    back = exchange(payload, GRP_DEV)

    mlp_own = mlp_piece(0)
    cross_own = cross_piece(0)
    pieces, own, hot_part = fold_first(
        here_of(1, core), mlp_own, cross_own, hot_part, mlp_came, cross_came
    )
    came = send_on(1, pieces)
    pieces, own, hot_part = fold_second(here_of(2, core), own, hot_part, came)
    came = send_on(2, pieces)
    wide = own.shape[1]
    sums = add_up(own, [c[:, :wide] for c in came])
    hot_part = jnp.concatenate([hot_part] + [c[:, wide:] for c in came])
    mlp_weight_grad = sums[:, :inputs]
    shared = jnp.broadcast_to(sums[None, :, inputs:].astype(BF16), (chips, 16, WIDE))
    shared = exchange(shared, CHIPS).reshape(-1, WIDE)
    hot_other = lax.ppermute(hot_part, CORE, SWAP)
    cold_grad = cold_sum(got, back, cold_table.shape[0])
    owners = hot_owners([lax.axis_index(axis) for axis in CHIPS], core)
    hot_grad = hot_sum(owners, got, hot_part, hot_other, hot_table.shape[0])
    other_shared = lax.ppermute(shared, CORE, SWAP)
    cross_u_grad, cross_v_grad, cross_bias_grad, mlp_bias_grad, out_weight_grad = unpack(
        core, shared, other_shared, inputs, rank, hidden_units
    )
    return (
        cold_grad,
        hot_grad,
        mlp_weight_grad,
        cross_u_grad,
        cross_v_grad,
        cross_bias_grad.reshape(-1),
        mlp_bias_grad.reshape(-1),
        out_weight_grad.reshape(-1),
    )


def solution(mesh):
    torus = Mesh(
        mesh.devices.reshape(mesh.shape["grp"], 4, 4, 2), ("grp", "dev_0", "dev_1", "dev_2")
    )
    placed = (
        P(GRP_DEV, None, None),
        P(),
        P(GRP_DEV, None),
        P(GRP_DEV, None),
        P(GRP_DEV, None),
        P(),
        P(GRP_DEV),
        P(),
        P(),
        P(),
        P(),
        P(),
        P(),
    )
    return jax.shard_map(
        per_device,
        mesh=torus,
        in_specs=placed,
        out_specs=(P(GRP_DEV, None), P(), P(GRP_DEV, None), P(), P(), P(), P(), P()),
        check_vma=False,
    )
```

```python
import jax
import jax.numpy as jnp
from jax import lax
from jax.experimental import pallas as pl
from jax.experimental.pallas import tpu as pltpu
from jax.sharding import Mesh
from jax.sharding import PartitionSpec as P


GRP_DEV = ("grp", "dev_0", "dev_1", "dev_2")
CHIPS = ("grp", "dev_0", "dev_1")
CORE = "dev_2"
SWAP = [(0, 1), (1, 0)]
ORDER = ((2, 1, 0), (0, 2, 1))
CAP = 40
HOT = 32
WIDE = 512
WAYS = 8
F32, BF16, I32 = jnp.float32, jnp.bfloat16, jnp.int32
VMEM = pl.BlockSpec(memory_space=pltpu.VMEM)
SMEM = pl.BlockSpec(memory_space=pltpu.SMEM)


def spread(x, ones):
    return jnp.dot(x.astype(F32).astype(BF16), ones, preferred_element_type=F32).astype(I32)


def route_kernel(ids, hot_list, ids_lanes, location, send, inverse, position, found):
    blocks = position.shape[0]
    features = blocks // 2

    def pick(b, carried):
        for j in range(128):
            found[pl.ds(b * 128 + j, 1), :] = location[pl.ds(ids[b, j] >> 7, 1), :]
        return carried

    lax.fori_loop(0, blocks, pick, 0)
    rows = lax.broadcasted_iota(I32, (128, 128), 0)
    lanes = lax.broadcasted_iota(I32, (128, 128), 1)
    before = (lanes < rows).astype(BF16)
    diagonal = rows == lanes
    ones = jnp.ones((128, 128), BF16)
    low = [
        spread(jnp.where(diagonal, ids_lanes[b : b + 1, :] & 127, 0), ones) for b in range(blocks)
    ]
    value = [
        jnp.where(low[b] == lanes, found[b * 128 : (b + 1) * 128, :], 0) for b in range(blocks)
    ]
    owner = [spread(v >> 11, ones) for v in value]
    high = [spread((v & 2047) >> 4, ones) for v in value]
    deep = [spread(v & 15, ones) for v in value]
    chosen = [o == lanes for o in owner]
    one_hot = [c.astype(F32).astype(BF16) for c in chosen]
    ahead = [jnp.dot(before, o, preferred_element_type=F32) for o in one_hot]
    seen = jnp.zeros((1, 128), F32)
    table = jnp.zeros((128, 256), F32)
    lane_rank = lanes & 63
    left = lanes < 64
    for b in range(blocks):
        rank = spread(jnp.where(chosen[b], ahead[b] + seen, 0.0), ones)
        seen = seen + ahead[b][127:, :] + chosen[b][127:, :].astype(F32)
        hit = lane_rank == rank
        origin = (b % features) * 128 + rows
        slots = jnp.where(hit, jnp.where(left, high[b], deep[b]), 0)
        origins = jnp.where(hit, jnp.where(left, origin >> 4, origin & 15), 0)
        marks = jnp.concatenate(
            [slots.astype(F32).astype(BF16), origins.astype(F32).astype(BF16)], axis=1
        )
        table = table + contract_rows(one_hot[b], marks)
        spot = jnp.where(diagonal, owner[b] * CAP + rank, 0)
        position[b : b + 1, :] = jnp.sum(spot, axis=0, keepdims=True)
    table = table.astype(I32)
    held = spread(jnp.where(diagonal, jnp.broadcast_to(seen, (128, 128)), 0.0), ones)
    wanted = (table[:, :64] << 4) + table[:, 64:128]
    wanted = jnp.where(lanes[:, :64] < held[:, :64], wanted, 2048)
    send[:, :CAP] = wanted[:, :CAP]
    send[:, CAP : CAP + HOT] = jnp.broadcast_to(hot_list[...], (128, HOT))
    send[:, CAP + HOT :] = jnp.zeros((128, 128 - CAP - HOT), I32)
    inverse[...] = (table[:, 128:192] << 4) + table[:, 192:256]


def route(ids, hot_list, location):
    blocks = ids.shape[0]
    return pl.pallas_call(
        route_kernel,
        out_shape=(
            jax.ShapeDtypeStruct((128, 128), I32),
            jax.ShapeDtypeStruct((128, 64), I32),
            jax.ShapeDtypeStruct((blocks, 128), I32),
        ),
        in_specs=[SMEM, VMEM, VMEM, VMEM],
        out_specs=(VMEM, VMEM, VMEM),
        scratch_shapes=[pltpu.VMEM((blocks * 128, 128), I32)],
        name="route",
    )(ids, hot_list, ids, location)


def fetch_kernel(wanted, table, out, wide, picked):
    shard = table.shape[0]
    wide[:shard, :] = table[...].astype(F32)
    wide[shard:, :] = jnp.zeros((8, 128), F32)

    def source(d, carried):
        for i in range(CAP):
            picked[pl.ds(d * CAP + i, 1), :] = wide[pl.ds(wanted[d, i], 1), :]
        return carried

    lax.fori_loop(0, out.shape[0] // CAP, source, 0)
    out[...] = picked[...].astype(BF16)


def fetch(wanted, table):
    count = wanted.shape[0] * CAP
    return pl.pallas_call(
        fetch_kernel,
        out_shape=jax.ShapeDtypeStruct((count, 128), BF16),
        in_specs=[SMEM, VMEM],
        out_specs=VMEM,
        scratch_shapes=[
            pltpu.VMEM((table.shape[0] + 8, 128), F32),
            pltpu.VMEM((count, 128), F32),
        ],
        name="fetch",
    )(wanted, table)


def hot_spread_kernel(hot_index, hot_rows, out):
    features, samples = hot_index.shape
    slots = lax.broadcasted_iota(I32, (HOT, samples), 0)
    for f in range(features):
        picked = (slots == hot_index[f : f + 1, :]).astype(F32).astype(BF16)
        out[f * samples : (f + 1) * samples, :] = contract_rows(picked, hot_rows[...])


def hot_spread(hot_index, hot_rows):
    return pl.pallas_call(
        hot_spread_kernel,
        out_shape=jax.ShapeDtypeStruct((hot_index.size, 128), F32),
        in_specs=[VMEM, VMEM],
        out_specs=VMEM,
        name="hot_spread",
    )(hot_index, hot_rows)


def pool_kernel(position, hot_part, arrived, out, wide, total):
    samples = total.shape[0]
    features = hot_part.shape[0] // samples
    wide[...] = arrived[...].astype(F32)

    def feature(f, carried):
        for s in range(samples):
            total[s : s + 1, :] = (
                wide[pl.ds(position[f, s], 1), :] + wide[pl.ds(position[features + f, s], 1), :]
            )
        at = pl.multiple_of(f * samples, samples)
        both = total[...] + hot_part[pl.ds(at, samples), :]
        out[:, pl.ds(pl.multiple_of(f * 128, 128), 128)] = both.astype(BF16)
        return carried

    lax.fori_loop(0, features, feature, 0)


def pool(position, hot_part, arrived):
    samples = position.shape[1]
    return pl.pallas_call(
        pool_kernel,
        out_shape=jax.ShapeDtypeStruct((samples, hot_part.shape[0] // samples * 128), BF16),
        in_specs=[SMEM, VMEM, VMEM],
        out_specs=VMEM,
        scratch_shapes=[pltpu.VMEM(arrived.shape, F32), pltpu.VMEM((samples, 128), F32)],
        name="pool",
    )(position, hot_part, arrived)


def pack_kernel(inverse, grad, out, wide, picked):
    samples, inputs = grad.shape
    devices = out.shape[0]
    for f in range(inputs // 128):
        part = grad[:, f * 128 : (f + 1) * 128]
        wide[f * samples : (f + 1) * samples, :] = part.astype(F32)

    def source(d, carried):
        for i in range(CAP):
            picked[pl.ds(d * CAP + i, 1), :] = wide[pl.ds(inverse[d, i], 1), :]
        return carried

    lax.fori_loop(0, devices, source, 0)
    out[...] = picked[...].reshape(devices, CAP, 128).astype(BF16)


def pack(inverse, grad):
    devices = inverse.shape[0]
    return pl.pallas_call(
        pack_kernel,
        out_shape=jax.ShapeDtypeStruct((devices, CAP, 128), BF16),
        in_specs=[SMEM, VMEM],
        out_specs=VMEM,
        scratch_shapes=[
            pltpu.VMEM((grad.size // 128, 128), F32),
            pltpu.VMEM((devices * CAP, 128), F32),
        ],
        name="pack",
    )(inverse, grad)


def hot_block_kernel(hot_index, grad, out):
    features, samples = hot_index.shape
    slots = lax.broadcasted_iota(I32, (HOT, samples), 0)
    one_hot = jnp.concatenate(
        [(slots == hot_index[f : f + 1, :]).astype(F32).astype(BF16) for f in range(features)],
        axis=1,
    )
    rows = jnp.concatenate([grad[:, f * 128 : (f + 1) * 128] for f in range(features)])
    total = jnp.dot(one_hot, rows, preferred_element_type=F32).astype(BF16)
    for b in range(HOT // 8):
        out[:, b * 128 : (b + 1) * 128] = total[b * 8 : (b + 1) * 8, :]


def hot_block(hot_index, grad):
    return pl.pallas_call(
        hot_block_kernel,
        out_shape=jax.ShapeDtypeStruct((8, HOT // 8 * 128), BF16),
        in_specs=[VMEM, VMEM],
        out_specs=VMEM,
        name="hot_block",
    )(hot_index, grad)


def cold_kernel(wanted, came, out, wide, *sums):
    for way in sums:
        way[...] = jnp.zeros(way.shape, F32)
    wide[...] = came[...].astype(F32)

    def source(d, carried):
        for i in range(CAP // WAYS):
            for k, way in enumerate(sums):
                at = k * (CAP // WAYS) + i
                here = pl.ds(wanted[d, at], 1)
                way[here, :] = way[here, :] + wide[d, at : at + 1, :]
        return carried

    lax.fori_loop(0, wide.shape[0], source, 0)
    shard = out.shape[0]
    total = sums[0][:shard, :]
    for way in sums[1:]:
        total = total + way[:shard, :]
    out[...] = total


def cold_sum(wanted, came, shard_rows):
    return pl.pallas_call(
        cold_kernel,
        out_shape=jax.ShapeDtypeStruct((shard_rows, 128), F32),
        in_specs=[SMEM, VMEM],
        out_specs=VMEM,
        scratch_shapes=[pltpu.VMEM((came.shape[0], CAP, 128), F32)]
        + [pltpu.VMEM((shard_rows + 8, 128), F32)] * WAYS,
        name="cold_sum",
    )(wanted, came)


def hot_kernel(owners, listed, held, came, out, wide_held, wide_came):
    out[...] = jnp.zeros(out.shape, F32)
    tall = held.shape[0]
    for b in range(held.shape[1] // 128):
        lanes = slice(b * 128, (b + 1) * 128)
        wide_held[b * tall : (b + 1) * tall, :] = held[:, lanes].astype(F32)
        wide_came[b * tall : (b + 1) * tall, :] = came[:, lanes].astype(F32)

    def source(k, carried):
        first, second, third = k >> 4, (k >> 2) & 3, k & 3
        base = (second * 8 + (first >> 1) * 2) * tall + third * 16 + (first & 1) * 8
        for side, wide in ((0, wide_held), (1, wide_came)):
            d = owners[side, k]
            places = [pl.ds(listed[d, CAP + i], 1) for i in range(HOT)]
            sums = []
            for i, here in enumerate(places):
                at = (i // 16 * 4 + i // 8 % 2) * tall + i % 8
                sums.append(out[here, :] + wide[pl.ds(base + at, 1), :])
            for here, row in zip(places, sums):
                out[here, :] = row
        return carried

    lax.fori_loop(0, 64, source, 0)


def hot_sum(owners, listed, held, came, hot_rows):
    return pl.pallas_call(
        hot_kernel,
        out_shape=jax.ShapeDtypeStruct((hot_rows, 128), F32),
        in_specs=[SMEM, SMEM, VMEM, VMEM],
        out_specs=VMEM,
        scratch_shapes=[pltpu.VMEM((held.size // 128, 128), F32)] * 2,
        name="hot_sum",
    )(owners, listed, held, came)


def hot_owners(spot, core):
    k = jnp.arange(64, dtype=I32)
    steps = [k >> 4, (k >> 2) & 3, k & 3]
    tables = []
    for c in range(2):
        place = [0, 0, 0]
        for axis, step in zip(ORDER[c], steps):
            back = jnp.where(step == 2, 3, jnp.where(step == 3, 2, step))
            place[axis] = (spot[axis] - back + 4) & 3
        tables.append(((place[0] * 4 + place[1]) * 4 + place[2]) * 2 + c)
    first = core == 0
    return jnp.stack(
        [jnp.where(first, tables[0], tables[1]), jnp.where(first, tables[1], tables[0])]
    )


def unpack_kernel(core, held, came, u_out, v_out, bias_out, mlp_bias_out, out_weight_out, wide):
    first = core[0] == 0
    rank = v_out.shape[0]

    def block(c, chip, lanes):
        here = slice(chip * 16, (chip + 1) * 16)
        own, other = held[here, lanes].astype(F32), came[here, lanes].astype(F32)
        return jnp.where(first, own, other) if c == 0 else jnp.where(first, other, own)

    def chip_of(c, spot):
        place = [0, 0, 0]
        for axis, at in zip(ORDER[c], spot):
            place[axis] = at
        return (place[0] * 4 + place[1]) * 4 + place[2]

    blocks = rank // 16
    for q in range(4):
        count = WIDE if q < 3 else v_out.shape[1] - 3 * WIDE
        for r in range(blocks):
            spot = (q, r // 4, r % 4)
            rows = slice(r * 16, (r + 1) * 16)
            wide[rows, :count] = block(0, chip_of(0, spot), slice(0, count))
            v_out[rows, q * WIDE : q * WIDE + count] = block(1, chip_of(1, spot), slice(0, count))
        u_out[q * WIDE : q * WIDE + count, :] = wide[:, :count].T

    lanes = slice(128, 256)
    sums = jnp.concatenate(
        [
            block(0, chip_of(0, (3, r // 4, r % 4)), lanes)
            + block(1, chip_of(1, (3, r // 4, r % 4)), lanes)
            for r in range(3)
        ]
    )
    bias_out[...] = sums[: bias_out.shape[0]]
    start = bias_out.shape[0]
    for out in (mlp_bias_out, out_weight_out):
        tall = out.shape[0]
        part = sums[start : start + tall]
        start += tall
        for c in range(2):
            for at in range(64):
                spot = (at // 16, at // 4 % 4, at % 4)
                chip = chip_of(c, spot)
                come, go = c * 64 + at, chip * 2 + c
                out[go // 8 : go // 8 + 1, go % 8 * 16 : go % 8 * 16 + 16] = part[
                    come // 8 : come // 8 + 1, come % 8 * 16 : come % 8 * 16 + 16
                ]


def unpack(core, held, came, inputs, rank, hidden_units):
    return pl.pallas_call(
        unpack_kernel,
        out_shape=(
            jax.ShapeDtypeStruct((inputs, rank), F32),
            jax.ShapeDtypeStruct((rank, inputs), F32),
            jax.ShapeDtypeStruct((inputs // 128, 128), F32),
            jax.ShapeDtypeStruct((hidden_units // 128, 128), F32),
            jax.ShapeDtypeStruct((hidden_units // 128, 128), F32),
        ),
        in_specs=[SMEM, VMEM, VMEM],
        out_specs=(VMEM,) * 5,
        scratch_shapes=[pltpu.VMEM((rank, WIDE), F32)],
        name="unpack",
    )(core.reshape(1), held, came)


def silu_slope(values):
    squash = jax.nn.sigmoid(values)
    return squash * (1.0 + values * (1.0 - squash))


def contract_rows(former, latter):
    return lax.dot_general(former, latter, (((0,), (0,)), ((), ())), preferred_element_type=F32)


def contract_cols(former, latter):
    return lax.dot_general(former, latter, (((1,), (1,)), ((), ())), preferred_element_type=F32)


def exchange(x, axes):
    return lax.all_to_all(x, axes, split_axis=0, concat_axis=0, tiled=True)


def route_pairs(phase, shift):
    pairs = []
    for d in range(128):
        spot = [d // 32, d // 8 % 4, d // 2 % 4]
        axis = ORDER[d % 2][phase]
        spot[axis] = (spot[axis] + shift) % 4
        pairs.append((d, ((spot[0] * 4 + spot[1]) * 4 + spot[2]) * 2 + d % 2))
    return pairs


SHIFTS = (1, 3, 2)


def here_of(phase, core):
    here = [lax.axis_index(CHIPS[ORDER[c][phase]]) for c in range(2)]
    return jnp.where(core == 0, here[0], here[1])


def send_on(phase, pieces):
    return [lax.ppermute(p, GRP_DEV, route_pairs(phase, s)) for p, s in zip(pieces, SHIFTS)]


def add_up(own, came):
    total = own.astype(F32)
    for part in came:
        total = total + part.astype(F32)
    return total


def fold_first_kernel(here, mlp, cross, hot, *refs):
    mlp_came, cross_came, (outs, own, hot_out, total) = refs[:3], refs[3:6], (
        refs[6:9],
        refs[9],
        refs[10],
        refs[11],
    )
    tall, inputs = mlp.shape
    part = mlp[...]
    for c in mlp_came:
        part = part + c[...].astype(F32)
    total[:, :inputs] = part
    part = cross[...]
    for c in cross_came:
        part = part + c[:tall, :].astype(F32)
    total[:, inputs:] = part
    blocks = [hot[...].astype(F32)] + [c[tall:, :].astype(F32) for c in cross_came]
    lanes = hot.shape[1] // 2
    hot_rows = jnp.concatenate(
        [b[:, :lanes] for b in blocks] + [b[:, lanes:] for b in blocks]
    ).astype(BF16)
    hot_out[...] = hot_rows
    count = tall // 4
    for out, s in zip(outs, SHIFTS):
        at = pl.multiple_of(((here[0] + s) & 3) * count, count)
        out[:, : total.shape[1]] = total[pl.ds(at, count), :].astype(BF16)
        out[:, total.shape[1] :] = hot_rows
    own[...] = total[pl.ds(pl.multiple_of(here[0] * count, count), count), :]


def fold_first(here, mlp, cross, hot, mlp_came, cross_came):
    tall, wide = mlp.shape[0], mlp.shape[1] + cross.shape[1]
    lanes = hot.shape[1] // 2
    out = jax.ShapeDtypeStruct((tall // 4, wide + lanes), BF16)
    got = pl.pallas_call(
        fold_first_kernel,
        out_shape=(out, out, out)
        + (
            jax.ShapeDtypeStruct((tall // 4, wide), F32),
            jax.ShapeDtypeStruct((tall // 4, lanes), BF16),
        ),
        in_specs=[SMEM] + [VMEM] * 9,
        out_specs=(VMEM,) * 5,
        scratch_shapes=[pltpu.VMEM((tall, wide), F32)],
        name="fold_first",
    )(here.reshape(1), mlp, cross, hot, *mlp_came, *cross_came)
    return got[:3], got[3], got[4]


def fold_second_kernel(here, own_in, hot, *refs):
    came, outs, own, hot_out, total = refs[:3], refs[3:6], refs[6], refs[7], refs[8]
    wide = own_in.shape[1]
    lanes = hot.shape[1]
    part = own_in[...]
    for c in came:
        part = part + c[:, :wide].astype(F32)
    total[...] = part
    blocks = [hot[...]] + [c[:, wide:] for c in came]
    for j, block in enumerate(blocks):
        for t in range(4):
            hot_out[:, (j * 4 + t) * lanes : (j * 4 + t + 1) * lanes] = block[t * 16 : t * 16 + 16]
    for out, s in zip(outs, SHIFTS):
        at = pl.multiple_of(((here[0] + s) & 3) * 16, 16)
        out[:, :wide] = total[pl.ds(at, 16), :].astype(BF16)
        out[:, wide:] = hot_out[...]
    own[...] = total[pl.ds(pl.multiple_of(here[0] * 16, 16), 16), :]


def fold_second(here, own, hot, came):
    wide, lanes = own.shape[1], 16 * hot.shape[1]
    out = jax.ShapeDtypeStruct((16, wide + lanes), BF16)
    got = pl.pallas_call(
        fold_second_kernel,
        out_shape=(out, out, out)
        + (jax.ShapeDtypeStruct((16, wide), F32), jax.ShapeDtypeStruct((16, lanes), BF16)),
        in_specs=[SMEM] + [VMEM] * 5,
        out_specs=(VMEM,) * 5,
        scratch_shapes=[pltpu.VMEM(own.shape, F32)],
        name="fold_second",
    )(here.reshape(1), own, hot, *came)
    return got[:3], got[3], got[4]


def by_core(x):
    parts = x.reshape(4, 4, 4, 2, 16, *x.shape[1:])
    halves = []
    for c in range(2):
        rest = tuple(range(3, 3 + x.ndim))
        half = parts[:, :, :, c].transpose(*ORDER[c], *rest)
        halves.append(half.reshape(-1, *x.shape[1:]))
    return jnp.concatenate(halves)


def per_device(
    ids,
    location,
    cold_table,
    hot_index,
    hot_list,
    hot_table,
    labels,
    cross_u,
    cross_v,
    cross_bias,
    mlp_weight,
    mlp_bias,
    out_weight,
):
    devices = lax.axis_size(GRP_DEV)
    chips = lax.axis_size(CHIPS)
    samples, features, bag_size = ids.shape
    width = cold_table.shape[1]
    hidden_units, inputs = mlp_weight.shape
    rank = cross_u.shape[1]
    core = lax.axis_index(CORE)

    ids_rows = ids.transpose(2, 1, 0).reshape(bag_size * features, samples)
    send, inverse, position = route(ids_rows, hot_list, location.reshape(-1, 128))
    got = exchange(send.reshape(devices, 1, 128), GRP_DEV).reshape(devices, 128)
    rows = fetch(got, cold_table)
    arrived = exchange(rows.reshape(devices, CAP, width), GRP_DEV)
    arrived = arrived.reshape(devices * CAP, width)

    mlp_weight = by_core(mlp_weight)
    mlp_bias = by_core(mlp_bias)
    out_weight = by_core(out_weight)
    hot_rows = hot_table[hot_list[0]]
    hot_index = hot_index.T
    first_input = pool(position, hot_spread(hot_index, hot_rows), arrived)
    cross_low = jnp.dot(first_input, cross_u, preferred_element_type=F32).astype(BF16)
    cross_term = jnp.dot(cross_low, cross_v, preferred_element_type=F32) + cross_bias
    input_wide = first_input.astype(F32)
    cross_out = (input_wide * cross_term + input_wide).astype(BF16)
    hidden_in = contract_cols(cross_out, mlp_weight) + mlp_bias
    hidden = jax.nn.silu(hidden_in).astype(BF16)
    logits = jnp.dot(hidden, out_weight, preferred_element_type=F32)
    logit_grad = jax.nn.sigmoid(logits) - labels.astype(F32)
    out_grad = jnp.sum(logit_grad[:, None] * hidden.astype(F32), axis=0)
    hidden_grad = (
        logit_grad[:, None] * out_weight.astype(F32)[None, :] * silu_slope(hidden_in)
    ).astype(BF16)
    bias_grad = jnp.sum(hidden_grad.astype(F32), axis=0)

    half = hidden_units // 2
    mine = lax.dynamic_slice(hidden_grad, (0, core * half), (samples, half))
    other = lax.dynamic_slice(hidden_grad, (0, (1 - core) * half), (samples, half))
    other = lax.ppermute(jnp.concatenate([other, cross_out], axis=1), CORE, SWAP)
    left = jnp.concatenate([mine, other[:, :half]], axis=0)
    right = jnp.concatenate([cross_out, other[:, half:]], axis=0)
    here = here_of(0, core)

    def mlp_piece(shift):
        at = (here + shift) % 4 * (half // 4)
        return contract_rows(lax.dynamic_slice_in_dim(left, at, half // 4, 1), right)

    cross_out_grad = jnp.dot(hidden_grad, mlp_weight, preferred_element_type=F32)
    term_grad = (cross_out_grad * input_wide).astype(BF16)
    cross_bias_part = jnp.sum(term_grad.astype(F32), axis=0)
    low_grad = contract_cols(term_grad, cross_v).astype(BF16)
    pooled_grad = (
        cross_out_grad * (cross_term + 1.0) + contract_cols(low_grad, cross_u)
    ).astype(BF16)

    mlp_came = send_on(0, [mlp_piece(s).astype(BF16) for s in SHIFTS])

    first = core == 0
    pad = jnp.zeros((samples, 4 * WIDE - inputs), BF16)
    pair_u = jnp.concatenate([low_grad, first_input, pad], axis=1)
    pair_v = jnp.concatenate([cross_low, term_grad, pad], axis=1)
    held = jnp.where(first, pair_u, pair_v)
    came = lax.ppermute(jnp.where(first, pair_v, pair_u), CORE, SWAP)
    both = jnp.concatenate([held, came], axis=0)
    vectors = jnp.concatenate([cross_bias_part, bias_grad, out_grad])
    vector_rows = vectors.size // 128
    start = inputs - 3 * WIDE
    vectors = jnp.pad(
        vectors.reshape(vector_rows, 128), ((0, rank - vector_rows), (start, WIDE - start - 128))
    )

    def cross_piece(shift):
        at = (here + shift) % 4
        part = lax.dynamic_slice_in_dim(both, rank + at * WIDE, WIDE, 1)
        return contract_rows(both[:, :rank], part) + jnp.where(at == 3, vectors, 0.0)

    hot_part = hot_block(hot_index, pooled_grad)
    cross_came = send_on(
        0, [jnp.concatenate([cross_piece(s).astype(BF16), hot_part]) for s in SHIFTS]
    )

    payload = pack(inverse, pooled_grad)
    back = exchange(payload, GRP_DEV)

    mlp_own = mlp_piece(0)
    cross_own = cross_piece(0)
    pieces, own, hot_part = fold_first(
        here_of(1, core), mlp_own, cross_own, hot_part, mlp_came, cross_came
    )
    came = send_on(1, pieces)
    pieces, own, hot_part = fold_second(here_of(2, core), own, hot_part, came)
    came = send_on(2, pieces)
    wide = own.shape[1]
    sums = add_up(own, [c[:, :wide] for c in came])
    hot_part = jnp.concatenate([hot_part] + [c[:, wide:] for c in came])
    mlp_weight_grad = sums[:, :inputs]
    shared = jnp.broadcast_to(sums[None, :, inputs:].astype(BF16), (chips, 16, WIDE))
    shared = exchange(shared, CHIPS).reshape(-1, WIDE)
    hot_other = lax.ppermute(hot_part, CORE, SWAP)
    cold_grad = cold_sum(got, back, cold_table.shape[0])
    owners = hot_owners([lax.axis_index(axis) for axis in CHIPS], core)
    hot_grad = hot_sum(owners, got, hot_part, hot_other, hot_table.shape[0])
    other_shared = lax.ppermute(shared, CORE, SWAP)
    cross_u_grad, cross_v_grad, cross_bias_grad, mlp_bias_grad, out_weight_grad = unpack(
        core, shared, other_shared, inputs, rank, hidden_units
    )
    return (
        cold_grad,
        hot_grad,
        mlp_weight_grad,
        cross_u_grad,
        cross_v_grad,
        cross_bias_grad.reshape(-1),
        mlp_bias_grad.reshape(-1),
        out_weight_grad.reshape(-1),
    )


def solution(mesh):
    torus = Mesh(
        mesh.devices.reshape(mesh.shape["grp"], 4, 4, 2), ("grp", "dev_0", "dev_1", "dev_2")
    )
    placed = (
        P(GRP_DEV, None, None),
        P(),
        P(GRP_DEV, None),
        P(GRP_DEV, None),
        P(GRP_DEV, None),
        P(),
        P(GRP_DEV),
        P(),
        P(),
        P(),
        P(),
        P(),
        P(),
    )
    return jax.shard_map(
        per_device,
        mesh=torus,
        in_specs=placed,
        out_specs=(P(GRP_DEV, None), P(), P(GRP_DEV, None), P(), P(), P(), P(), P()),
        check_vma=False,
    )
```

```python
import jax
import jax.numpy as jnp
from jax import lax
from jax.experimental import pallas as pl
from jax.experimental.pallas import tpu as pltpu
from jax.sharding import Mesh
from jax.sharding import PartitionSpec as P


GRP_DEV = ("grp", "dev_0", "dev_1", "dev_2")
CHIPS = ("grp", "dev_0", "dev_1")
CORE = "dev_2"
SWAP = [(0, 1), (1, 0)]
ORDER = ((2, 1, 0), (0, 2, 1))
CAP = 40
HOT = 32
WIDE = 512
WAYS = 8
F32, BF16, I32 = jnp.float32, jnp.bfloat16, jnp.int32
VMEM = pl.BlockSpec(memory_space=pltpu.VMEM)
SMEM = pl.BlockSpec(memory_space=pltpu.SMEM)


def spread(x, ones):
    return jnp.dot(x.astype(F32).astype(BF16), ones, preferred_element_type=F32).astype(I32)


def route_kernel(ids, hot_list, ids_lanes, location, send, inverse, position, found):
    blocks = position.shape[0]
    features = blocks // 2

    def pick(b, carried):
        for j in range(128):
            found[pl.ds(b * 128 + j, 1), :] = location[pl.ds(ids[b, j] >> 7, 1), :]
        return carried

    lax.fori_loop(0, blocks, pick, 0)
    rows = lax.broadcasted_iota(I32, (128, 128), 0)
    lanes = lax.broadcasted_iota(I32, (128, 128), 1)
    before = (lanes < rows).astype(BF16)
    diagonal = rows == lanes
    ones = jnp.ones((128, 128), BF16)
    low = [
        spread(jnp.where(diagonal, ids_lanes[b : b + 1, :] & 127, 0), ones) for b in range(blocks)
    ]
    value = [
        jnp.where(low[b] == lanes, found[b * 128 : (b + 1) * 128, :], 0) for b in range(blocks)
    ]
    owner = [spread(v >> 11, ones) for v in value]
    high = [spread((v & 2047) >> 4, ones) for v in value]
    deep = [spread(v & 15, ones) for v in value]
    chosen = [o == lanes for o in owner]
    one_hot = [c.astype(F32).astype(BF16) for c in chosen]
    ahead = [jnp.dot(before, o, preferred_element_type=F32) for o in one_hot]
    seen = jnp.zeros((1, 128), F32)
    table = jnp.zeros((128, 256), F32)
    lane_rank = lanes & 63
    left = lanes < 64
    for b in range(blocks):
        rank = spread(jnp.where(chosen[b], ahead[b] + seen, 0.0), ones)
        seen = seen + ahead[b][127:, :] + chosen[b][127:, :].astype(F32)
        hit = lane_rank == rank
        origin = (b % features) * 128 + rows
        slots = jnp.where(hit, jnp.where(left, high[b], deep[b]), 0)
        origins = jnp.where(hit, jnp.where(left, origin >> 4, origin & 15), 0)
        marks = jnp.concatenate(
            [slots.astype(F32).astype(BF16), origins.astype(F32).astype(BF16)], axis=1
        )
        table = table + contract_rows(one_hot[b], marks)
        spot = jnp.where(diagonal, owner[b] * CAP + rank, 0)
        position[b : b + 1, :] = jnp.sum(spot, axis=0, keepdims=True)
    table = table.astype(I32)
    held = spread(jnp.where(diagonal, jnp.broadcast_to(seen, (128, 128)), 0.0), ones)
    wanted = (table[:, :64] << 4) + table[:, 64:128]
    wanted = jnp.where(lanes[:, :64] < held[:, :64], wanted, 2048)
    send[:, :CAP] = wanted[:, :CAP]
    send[:, CAP : CAP + HOT] = jnp.broadcast_to(hot_list[...], (128, HOT))
    send[:, CAP + HOT :] = jnp.zeros((128, 128 - CAP - HOT), I32)
    inverse[...] = (table[:, 128:192] << 4) + table[:, 192:256]


def route(ids, hot_list, location):
    blocks = ids.shape[0]
    return pl.pallas_call(
        route_kernel,
        out_shape=(
            jax.ShapeDtypeStruct((128, 128), I32),
            jax.ShapeDtypeStruct((128, 64), I32),
            jax.ShapeDtypeStruct((blocks, 128), I32),
        ),
        in_specs=[SMEM, VMEM, VMEM, VMEM],
        out_specs=(VMEM, VMEM, VMEM),
        scratch_shapes=[pltpu.VMEM((blocks * 128, 128), I32)],
        name="route",
    )(ids, hot_list, ids, location)


def fetch_kernel(wanted, table, out, wide, picked):
    shard = table.shape[0]
    wide[:shard, :] = table[...].astype(F32)
    wide[shard:, :] = jnp.zeros((8, 128), F32)

    def source(d, carried):
        for i in range(CAP):
            picked[pl.ds(d * CAP + i, 1), :] = wide[pl.ds(wanted[d, i], 1), :]
        return carried

    lax.fori_loop(0, out.shape[0] // CAP, source, 0)
    out[...] = picked[...].astype(BF16)


def fetch(wanted, table):
    count = wanted.shape[0] * CAP
    return pl.pallas_call(
        fetch_kernel,
        out_shape=jax.ShapeDtypeStruct((count, 128), BF16),
        in_specs=[SMEM, VMEM],
        out_specs=VMEM,
        scratch_shapes=[
            pltpu.VMEM((table.shape[0] + 8, 128), F32),
            pltpu.VMEM((count, 128), F32),
        ],
        name="fetch",
    )(wanted, table)


def hot_spread_kernel(hot_index, hot_rows, out):
    features, samples = hot_index.shape
    slots = lax.broadcasted_iota(I32, (HOT, samples), 0)
    for f in range(features):
        picked = (slots == hot_index[f : f + 1, :]).astype(F32).astype(BF16)
        out[f * samples : (f + 1) * samples, :] = contract_rows(picked, hot_rows[...])


def hot_spread(hot_index, hot_rows):
    return pl.pallas_call(
        hot_spread_kernel,
        out_shape=jax.ShapeDtypeStruct((hot_index.size, 128), F32),
        in_specs=[VMEM, VMEM],
        out_specs=VMEM,
        name="hot_spread",
    )(hot_index, hot_rows)


def pool_kernel(position, hot_part, arrived, out, wide, total):
    samples = total.shape[0]
    features = hot_part.shape[0] // samples
    wide[...] = arrived[...].astype(F32)

    def feature(f, carried):
        for s in range(samples):
            total[s : s + 1, :] = (
                wide[pl.ds(position[f, s], 1), :] + wide[pl.ds(position[features + f, s], 1), :]
            )
        at = pl.multiple_of(f * samples, samples)
        both = total[...] + hot_part[pl.ds(at, samples), :]
        out[:, pl.ds(pl.multiple_of(f * 128, 128), 128)] = both.astype(BF16)
        return carried

    lax.fori_loop(0, features, feature, 0)


def pool(position, hot_part, arrived):
    samples = position.shape[1]
    return pl.pallas_call(
        pool_kernel,
        out_shape=jax.ShapeDtypeStruct((samples, hot_part.shape[0] // samples * 128), BF16),
        in_specs=[SMEM, VMEM, VMEM],
        out_specs=VMEM,
        scratch_shapes=[pltpu.VMEM(arrived.shape, F32), pltpu.VMEM((samples, 128), F32)],
        name="pool",
    )(position, hot_part, arrived)


def pack_kernel(inverse, grad, out, wide, picked):
    samples, inputs = grad.shape
    devices = out.shape[0]
    for f in range(inputs // 128):
        part = grad[:, f * 128 : (f + 1) * 128]
        wide[f * samples : (f + 1) * samples, :] = part.astype(F32)

    def source(d, carried):
        for i in range(CAP):
            picked[pl.ds(d * CAP + i, 1), :] = wide[pl.ds(inverse[d, i], 1), :]
        return carried

    lax.fori_loop(0, devices, source, 0)
    out[...] = picked[...].reshape(devices, CAP, 128).astype(BF16)


def pack(inverse, grad):
    devices = inverse.shape[0]
    return pl.pallas_call(
        pack_kernel,
        out_shape=jax.ShapeDtypeStruct((devices, CAP, 128), BF16),
        in_specs=[SMEM, VMEM],
        out_specs=VMEM,
        scratch_shapes=[
            pltpu.VMEM((grad.size // 128, 128), F32),
            pltpu.VMEM((devices * CAP, 128), F32),
        ],
        name="pack",
    )(inverse, grad)


def hot_block_kernel(hot_index, grad, out):
    features, samples = hot_index.shape
    slots = lax.broadcasted_iota(I32, (HOT, samples), 0)
    one_hot = jnp.concatenate(
        [(slots == hot_index[f : f + 1, :]).astype(F32).astype(BF16) for f in range(features)],
        axis=1,
    )
    rows = jnp.concatenate([grad[:, f * 128 : (f + 1) * 128] for f in range(features)])
    total = jnp.dot(one_hot, rows, preferred_element_type=F32).astype(BF16)
    for b in range(HOT // 8):
        out[:, b * 128 : (b + 1) * 128] = total[b * 8 : (b + 1) * 8, :]


def hot_block(hot_index, grad):
    return pl.pallas_call(
        hot_block_kernel,
        out_shape=jax.ShapeDtypeStruct((8, HOT // 8 * 128), BF16),
        in_specs=[VMEM, VMEM],
        out_specs=VMEM,
        name="hot_block",
    )(hot_index, grad)


def cold_kernel(start, wanted, came, *refs):
    base, (out, wide, *sums) = (refs[0], refs[1:]) if start else (None, refs)
    count = wide.shape[0]
    for way in sums:
        way[...] = jnp.zeros(way.shape, F32)
    wide[...] = came[start : start + count, :, :].astype(F32)

    def source(d, carried):
        for i in range(CAP // WAYS):
            for k, way in enumerate(sums):
                at = k * (CAP // WAYS) + i
                here = pl.ds(wanted[start + d, at], 1)
                way[here, :] = way[here, :] + wide[d, at : at + 1, :]
        return carried

    lax.fori_loop(0, count, source, 0)
    shard = out.shape[0]
    total = sums[0][:shard, :]
    for way in sums[1:]:
        total = total + way[:shard, :]
    out[...] = total + base[...] if start else total


def cold_sum(wanted, came, shard_rows, base=()):
    half = came.shape[0] // 2
    start = half if base else 0
    return pl.pallas_call(
        lambda *refs: cold_kernel(start, *refs),
        out_shape=jax.ShapeDtypeStruct((shard_rows, 128), F32),
        in_specs=[SMEM, VMEM] + [VMEM] * len(base),
        out_specs=VMEM,
        scratch_shapes=[pltpu.VMEM((half, CAP, 128), F32)]
        + [pltpu.VMEM((shard_rows + 8, 128), F32)] * WAYS,
        name="cold_last" if base else "cold_first",
    )(wanted, came, *base)


def hot_kernel(owners, listed, held, came, out, wide_held, wide_came):
    out[...] = jnp.zeros(out.shape, F32)
    tall = held.shape[0]
    for b in range(held.shape[1] // 128):
        lanes = slice(b * 128, (b + 1) * 128)
        wide_held[b * tall : (b + 1) * tall, :] = held[:, lanes].astype(F32)
        wide_came[b * tall : (b + 1) * tall, :] = came[:, lanes].astype(F32)

    def source(k, carried):
        first, second, third = k >> 4, (k >> 2) & 3, k & 3
        base = (second * 8 + (first >> 1) * 2) * tall + third * 16 + (first & 1) * 8
        for side, wide in ((0, wide_held), (1, wide_came)):
            d = owners[side, k]
            places = [pl.ds(listed[d, CAP + i], 1) for i in range(HOT)]
            sums = []
            for i, here in enumerate(places):
                at = (i // 16 * 4 + i // 8 % 2) * tall + i % 8
                sums.append(out[here, :] + wide[pl.ds(base + at, 1), :])
            for here, row in zip(places, sums):
                out[here, :] = row
        return carried

    lax.fori_loop(0, 64, source, 0)


def hot_sum(owners, listed, held, came, hot_rows):
    return pl.pallas_call(
        hot_kernel,
        out_shape=jax.ShapeDtypeStruct((hot_rows, 128), F32),
        in_specs=[SMEM, SMEM, VMEM, VMEM],
        out_specs=VMEM,
        scratch_shapes=[pltpu.VMEM((held.size // 128, 128), F32)] * 2,
        name="hot_sum",
    )(owners, listed, held, came)


def hot_owners(spot, core):
    k = jnp.arange(64, dtype=I32)
    steps = [k >> 4, (k >> 2) & 3, k & 3]
    tables = []
    for c in range(2):
        place = [0, 0, 0]
        for axis, step in zip(ORDER[c], steps):
            back = jnp.where(step == 2, 3, jnp.where(step == 3, 2, step))
            place[axis] = (spot[axis] - back + 4) & 3
        tables.append(((place[0] * 4 + place[1]) * 4 + place[2]) * 2 + c)
    first = core == 0
    return jnp.stack(
        [jnp.where(first, tables[0], tables[1]), jnp.where(first, tables[1], tables[0])]
    )


def unpack_kernel(core, held, came, u_out, v_out, bias_out, mlp_bias_out, out_weight_out, wide):
    first = core[0] == 0
    rank = v_out.shape[0]

    def block(c, chip, lanes):
        here = slice(chip * 16, (chip + 1) * 16)
        own, other = held[here, lanes].astype(F32), came[here, lanes].astype(F32)
        return jnp.where(first, own, other) if c == 0 else jnp.where(first, other, own)

    def chip_of(c, spot):
        place = [0, 0, 0]
        for axis, at in zip(ORDER[c], spot):
            place[axis] = at
        return (place[0] * 4 + place[1]) * 4 + place[2]

    blocks = rank // 16
    for q in range(4):
        count = WIDE if q < 3 else v_out.shape[1] - 3 * WIDE
        for r in range(blocks):
            spot = (q, r // 4, r % 4)
            rows = slice(r * 16, (r + 1) * 16)
            wide[rows, :count] = block(0, chip_of(0, spot), slice(0, count))
            v_out[rows, q * WIDE : q * WIDE + count] = block(1, chip_of(1, spot), slice(0, count))
        u_out[q * WIDE : q * WIDE + count, :] = wide[:, :count].T

    lanes = slice(128, 256)
    sums = jnp.concatenate(
        [
            block(0, chip_of(0, (3, r // 4, r % 4)), lanes)
            + block(1, chip_of(1, (3, r // 4, r % 4)), lanes)
            for r in range(3)
        ]
    )
    bias_out[...] = sums[: bias_out.shape[0]]
    start = bias_out.shape[0]
    for out in (mlp_bias_out, out_weight_out):
        tall = out.shape[0]
        part = sums[start : start + tall]
        start += tall
        for c in range(2):
            for at in range(64):
                spot = (at // 16, at // 4 % 4, at % 4)
                chip = chip_of(c, spot)
                come, go = c * 64 + at, chip * 2 + c
                out[go // 8 : go // 8 + 1, go % 8 * 16 : go % 8 * 16 + 16] = part[
                    come // 8 : come // 8 + 1, come % 8 * 16 : come % 8 * 16 + 16
                ]


def unpack(core, held, came, inputs, rank, hidden_units):
    return pl.pallas_call(
        unpack_kernel,
        out_shape=(
            jax.ShapeDtypeStruct((inputs, rank), F32),
            jax.ShapeDtypeStruct((rank, inputs), F32),
            jax.ShapeDtypeStruct((inputs // 128, 128), F32),
            jax.ShapeDtypeStruct((hidden_units // 128, 128), F32),
            jax.ShapeDtypeStruct((hidden_units // 128, 128), F32),
        ),
        in_specs=[SMEM, VMEM, VMEM],
        out_specs=(VMEM,) * 5,
        scratch_shapes=[pltpu.VMEM((rank, WIDE), F32)],
        name="unpack",
    )(core.reshape(1), held, came)


def silu_slope(values):
    squash = jax.nn.sigmoid(values)
    return squash * (1.0 + values * (1.0 - squash))


def contract_rows(former, latter):
    return lax.dot_general(former, latter, (((0,), (0,)), ((), ())), preferred_element_type=F32)


def contract_cols(former, latter):
    return lax.dot_general(former, latter, (((1,), (1,)), ((), ())), preferred_element_type=F32)


def exchange(x, axes):
    return lax.all_to_all(x, axes, split_axis=0, concat_axis=0, tiled=True)


def route_pairs(phase, shift):
    pairs = []
    for d in range(128):
        spot = [d // 32, d // 8 % 4, d // 2 % 4]
        axis = ORDER[d % 2][phase]
        spot[axis] = (spot[axis] + shift) % 4
        pairs.append((d, ((spot[0] * 4 + spot[1]) * 4 + spot[2]) * 2 + d % 2))
    return pairs


SHIFTS = (1, 3, 2)


def here_of(phase, core):
    here = [lax.axis_index(CHIPS[ORDER[c][phase]]) for c in range(2)]
    return jnp.where(core == 0, here[0], here[1])


def send_on(phase, pieces):
    return [lax.ppermute(p, GRP_DEV, route_pairs(phase, s)) for p, s in zip(pieces, SHIFTS)]


def add_up(own, came):
    total = own.astype(F32)
    for part in came:
        total = total + part.astype(F32)
    return total


def fold_first_kernel(here, mlp, cross, hot, *refs):
    mlp_came, cross_came, (outs, own, hot_out, total) = refs[:3], refs[3:6], (
        refs[6:9],
        refs[9],
        refs[10],
        refs[11],
    )
    tall, inputs = mlp.shape
    part = mlp[...]
    for c in mlp_came:
        part = part + c[...].astype(F32)
    total[:, :inputs] = part
    part = cross[...]
    for c in cross_came:
        part = part + c[:tall, :].astype(F32)
    total[:, inputs:] = part
    blocks = [hot[...].astype(F32)] + [c[tall:, :].astype(F32) for c in cross_came]
    lanes = hot.shape[1] // 2
    hot_rows = jnp.concatenate(
        [b[:, :lanes] for b in blocks] + [b[:, lanes:] for b in blocks]
    ).astype(BF16)
    hot_out[...] = hot_rows
    count = tall // 4
    for out, s in zip(outs, SHIFTS):
        at = pl.multiple_of(((here[0] + s) & 3) * count, count)
        out[:, : total.shape[1]] = total[pl.ds(at, count), :].astype(BF16)
        out[:, total.shape[1] :] = hot_rows
    own[...] = total[pl.ds(pl.multiple_of(here[0] * count, count), count), :]


def fold_first(here, mlp, cross, hot, mlp_came, cross_came):
    tall, wide = mlp.shape[0], mlp.shape[1] + cross.shape[1]
    lanes = hot.shape[1] // 2
    out = jax.ShapeDtypeStruct((tall // 4, wide + lanes), BF16)
    got = pl.pallas_call(
        fold_first_kernel,
        out_shape=(out, out, out)
        + (
            jax.ShapeDtypeStruct((tall // 4, wide), F32),
            jax.ShapeDtypeStruct((tall // 4, lanes), BF16),
        ),
        in_specs=[SMEM] + [VMEM] * 9,
        out_specs=(VMEM,) * 5,
        scratch_shapes=[pltpu.VMEM((tall, wide), F32)],
        name="fold_first",
    )(here.reshape(1), mlp, cross, hot, *mlp_came, *cross_came)
    return got[:3], got[3], got[4]


def fold_second_kernel(here, own_in, hot, *refs):
    came, outs, own, hot_out, total = refs[:3], refs[3:6], refs[6], refs[7], refs[8]
    wide = own_in.shape[1]
    lanes = hot.shape[1]
    part = own_in[...]
    for c in came:
        part = part + c[:, :wide].astype(F32)
    total[...] = part
    blocks = [hot[...]] + [c[:, wide:] for c in came]
    for j, block in enumerate(blocks):
        for t in range(4):
            hot_out[:, (j * 4 + t) * lanes : (j * 4 + t + 1) * lanes] = block[t * 16 : t * 16 + 16]
    for out, s in zip(outs, SHIFTS):
        at = pl.multiple_of(((here[0] + s) & 3) * 16, 16)
        out[:, :wide] = total[pl.ds(at, 16), :].astype(BF16)
        out[:, wide:] = hot_out[...]
    own[...] = total[pl.ds(pl.multiple_of(here[0] * 16, 16), 16), :]


def fold_second(here, own, hot, came):
    wide, lanes = own.shape[1], 16 * hot.shape[1]
    out = jax.ShapeDtypeStruct((16, wide + lanes), BF16)
    got = pl.pallas_call(
        fold_second_kernel,
        out_shape=(out, out, out)
        + (jax.ShapeDtypeStruct((16, wide), F32), jax.ShapeDtypeStruct((16, lanes), BF16)),
        in_specs=[SMEM] + [VMEM] * 5,
        out_specs=(VMEM,) * 5,
        scratch_shapes=[pltpu.VMEM(own.shape, F32)],
        name="fold_second",
    )(here.reshape(1), own, hot, *came)
    return got[:3], got[3], got[4]


def by_core(x):
    parts = x.reshape(4, 4, 4, 2, 16, *x.shape[1:])
    halves = []
    for c in range(2):
        rest = tuple(range(3, 3 + x.ndim))
        half = parts[:, :, :, c].transpose(*ORDER[c], *rest)
        halves.append(half.reshape(-1, *x.shape[1:]))
    return jnp.concatenate(halves)


def per_device(
    ids,
    location,
    cold_table,
    hot_index,
    hot_list,
    hot_table,
    labels,
    cross_u,
    cross_v,
    cross_bias,
    mlp_weight,
    mlp_bias,
    out_weight,
):
    devices = lax.axis_size(GRP_DEV)
    chips = lax.axis_size(CHIPS)
    samples, features, bag_size = ids.shape
    width = cold_table.shape[1]
    hidden_units, inputs = mlp_weight.shape
    rank = cross_u.shape[1]
    core = lax.axis_index(CORE)

    ids_rows = ids.transpose(2, 1, 0).reshape(bag_size * features, samples)
    send, inverse, position = route(ids_rows, hot_list, location.reshape(-1, 128))
    got = exchange(send.reshape(devices, 1, 128), GRP_DEV).reshape(devices, 128)
    rows = fetch(got, cold_table)
    arrived = exchange(rows.reshape(devices, CAP, width), GRP_DEV)
    arrived = arrived.reshape(devices * CAP, width)

    mlp_weight = by_core(mlp_weight)
    mlp_bias = by_core(mlp_bias)
    out_weight = by_core(out_weight)
    hot_rows = hot_table[hot_list[0]]
    hot_index = hot_index.T
    first_input = pool(position, hot_spread(hot_index, hot_rows), arrived)
    cross_low = jnp.dot(first_input, cross_u, preferred_element_type=F32).astype(BF16)
    cross_term = jnp.dot(cross_low, cross_v, preferred_element_type=F32) + cross_bias
    input_wide = first_input.astype(F32)
    cross_out = (input_wide * cross_term + input_wide).astype(BF16)
    hidden_in = contract_cols(cross_out, mlp_weight) + mlp_bias
    hidden = jax.nn.silu(hidden_in).astype(BF16)
    logits = jnp.dot(hidden, out_weight, preferred_element_type=F32)
    logit_grad = jax.nn.sigmoid(logits) - labels.astype(F32)
    out_grad = jnp.dot(logit_grad, hidden.astype(F32), precision=lax.Precision.HIGHEST)
    hidden_grad = (
        logit_grad[:, None] * out_weight.astype(F32)[None, :] * silu_slope(hidden_in)
    ).astype(BF16)
    bias_grad = jnp.sum(hidden_grad.astype(F32), axis=0)

    half = hidden_units // 2
    mine = lax.dynamic_slice(hidden_grad, (0, core * half), (samples, half))
    other = lax.dynamic_slice(hidden_grad, (0, (1 - core) * half), (samples, half))
    other = lax.ppermute(jnp.concatenate([other, cross_out], axis=1), CORE, SWAP)
    left = jnp.concatenate([mine, other[:, :half]], axis=0)
    right = jnp.concatenate([cross_out, other[:, half:]], axis=0)
    here = here_of(0, core)

    def mlp_piece(shift):
        at = (here + shift) % 4 * (half // 4)
        return contract_rows(lax.dynamic_slice_in_dim(left, at, half // 4, 1), right)

    cross_out_grad = jnp.dot(hidden_grad, mlp_weight, preferred_element_type=F32)
    term_grad = (cross_out_grad * input_wide).astype(BF16)
    cross_bias_part = jnp.sum(term_grad.astype(F32), axis=0)
    low_grad = contract_cols(term_grad, cross_v).astype(BF16)
    pooled_grad = (
        cross_out_grad * (cross_term + 1.0) + contract_cols(low_grad, cross_u)
    ).astype(BF16)

    mlp_came = send_on(0, [mlp_piece(s).astype(BF16) for s in SHIFTS])

    first = core == 0
    pad = jnp.zeros((samples, 4 * WIDE - inputs), BF16)
    pair_u = jnp.concatenate([low_grad, first_input, pad], axis=1)
    pair_v = jnp.concatenate([cross_low, term_grad, pad], axis=1)
    held = jnp.where(first, pair_u, pair_v)
    came = lax.ppermute(jnp.where(first, pair_v, pair_u), CORE, SWAP)
    both = jnp.concatenate([held, came], axis=0)
    vectors = jnp.concatenate([cross_bias_part, bias_grad, out_grad])
    vector_rows = vectors.size // 128
    start = inputs - 3 * WIDE
    vectors = jnp.pad(
        vectors.reshape(vector_rows, 128), ((0, rank - vector_rows), (start, WIDE - start - 128))
    )

    def cross_piece(shift):
        at = (here + shift) % 4
        part = lax.dynamic_slice_in_dim(both, rank + at * WIDE, WIDE, 1)
        return contract_rows(both[:, :rank], part) + jnp.where(at == 3, vectors, 0.0)

    hot_part = hot_block(hot_index, pooled_grad)
    cross_came = send_on(
        0, [jnp.concatenate([cross_piece(s).astype(BF16), hot_part]) for s in SHIFTS]
    )

    payload = pack(inverse, pooled_grad)
    back = exchange(payload, GRP_DEV)

    mlp_own = mlp_piece(0)
    cross_own = cross_piece(0)
    pieces, own, hot_part = fold_first(
        here_of(1, core), mlp_own, cross_own, hot_part, mlp_came, cross_came
    )
    came = send_on(1, pieces)
    pieces, own, hot_part = fold_second(here_of(2, core), own, hot_part, came)
    came = send_on(2, pieces)
    wide = own.shape[1]
    sums = add_up(own, [c[:, :wide] for c in came])
    hot_part = jnp.concatenate([hot_part] + [c[:, wide:] for c in came])
    mlp_weight_grad = sums[:, :inputs]
    shared = jnp.broadcast_to(sums[None, :, inputs:].astype(BF16), (chips, 16, WIDE))
    shared = exchange(shared, CHIPS).reshape(-1, WIDE)
    hot_other = lax.ppermute(hot_part, CORE, SWAP)
    cold_half = cold_sum(got, back, cold_table.shape[0])
    cold_grad = cold_sum(got, back, cold_table.shape[0], (cold_half,))
    owners = hot_owners([lax.axis_index(axis) for axis in CHIPS], core)
    hot_grad = hot_sum(owners, got, hot_part, hot_other, hot_table.shape[0])
    other_shared = lax.ppermute(shared, CORE, SWAP)
    cross_u_grad, cross_v_grad, cross_bias_grad, mlp_bias_grad, out_weight_grad = unpack(
        core, shared, other_shared, inputs, rank, hidden_units
    )
    return (
        cold_grad,
        hot_grad,
        mlp_weight_grad,
        cross_u_grad,
        cross_v_grad,
        cross_bias_grad.reshape(-1),
        mlp_bias_grad.reshape(-1),
        out_weight_grad.reshape(-1),
    )


def solution(mesh):
    torus = Mesh(
        mesh.devices.reshape(mesh.shape["grp"], 4, 4, 2), ("grp", "dev_0", "dev_1", "dev_2")
    )
    placed = (
        P(GRP_DEV, None, None),
        P(),
        P(GRP_DEV, None),
        P(GRP_DEV, None),
        P(GRP_DEV, None),
        P(),
        P(GRP_DEV),
        P(),
        P(),
        P(),
        P(),
        P(),
        P(),
    )
    return jax.shard_map(
        per_device,
        mesh=torus,
        in_specs=placed,
        out_specs=(P(GRP_DEV, None), P(), P(GRP_DEV, None), P(), P(), P(), P(), P()),
        check_vma=False,
    )
```
